512 devices in a mesh: dp: 16 (over y_lo, x), ctx: 32 (over y_hi, z, core).
Axes of the slice: x: 4, y: 8 (y_hi: 2, y_lo: 4; y = y_hi * 4 + y_lo), z: 8, core: 2. Of those that a mesh axis runs over, the one named last changes fastest.
Arguments:
- query_rows: bfloat16 [65536, 4096], P(('dp', 'ctx')), may hold values from -32 to 32
- key_rows: bfloat16 [65536, 512], P(('dp', 'ctx')), may hold values from -8 to 8
- value_rows: bfloat16 [65536, 512], P(('dp', 'ctx')), may hold values from -6 to 6
- out_grad: bfloat16 [65536, 4096], P(('dp', 'ctx')), may hold values from -24 to 24
- destination: int32 [16, 4096], P('dp'), may hold values from 0 to 4095, as said below
- group_first: int32 [16, 32], P('dp', 'ctx'), may hold values from 0 to 31, as said below
Outputs:
- attended: bfloat16 [65536, 4096], P(('dp', 'ctx'))
- grad_query: bfloat16 [65536, 4096], P(('dp', 'ctx'))
- grad_key: bfloat16 [65536, 512], P(('dp', 'ctx'))
- grad_value: bfloat16 [65536, 512], P(('dp', 'ctx'))
- bias_grad: float32 [4608], replicated
The draws below stay inside these ranges and needn't reach their ends.
Inputs may be any that keep to these rules, and one draw needn't show every extreme that they name: For each replica r, destination[r] is a permutation of 0 to 4095. Of the 128 tokens of one index of ctx, at most 8 take slots in any one block, and in every replica some index and block reach 8. group_first[r, b] equals b where a sequence group begins (always at b = 0) and group_first[r, b - 1] otherwise.
All inputs are finite; a program needn't handle non-finite values.
Results may differ from the reference program's by a relative error of at most 0.008.
Values may be sent and summed in bfloat16 or wider, within the bound.
A program may use at most 64 MiB of HBM per device.

```python
import jax
import jax.numpy as jnp
from jax import lax

ROWS = 128
HD = 128
KVH = 4
GROUP = 8
RUN = 4096
TOKENS = 65536
N_DP = 16
N_CTX = 32


def replica_plan(stream):
    count = N_CTX
    share = ROWS // N_CTX
    parts = jax.random.split(stream, 6)
    order = jax.random.permutation(parts[0], count)
    shifts = jax.random.permutation(parts[1], count)
    spread = jax.random.randint(parts[2], (count // 2,), 0, share + 1).at[0].set(share)
    sizes = jnp.concatenate([share + spread, share - spread])
    sizes = sizes[jax.random.permutation(parts[3], count)]
    ends = jnp.cumsum(sizes)
    places = jnp.arange(ROWS)
    rounds = jnp.sum((places[None, :] >= ends[:, None]).astype(jnp.int32), axis=0)

    def shuffled(stream_one):
        return jax.random.permutation(stream_one, ROWS)
    row_order = jax.vmap(shuffled)(jax.random.split(parts[4], count))
    slot_order = jax.vmap(shuffled)(jax.random.split(parts[5], count))
    ranked = jnp.arange(count)
    sender = order[:, None] + jnp.zeros((1, ROWS), jnp.int32)
    target = order[(ranked[:, None] + shifts[rounds][None, :]) % count]
    values = target * ROWS + slot_order[target, places[None, :]]
    positions = sender * ROWS + row_order[sender, places[None, :]]
    empty = jnp.zeros((count * ROWS,), jnp.int32)
    return empty.at[positions.reshape(-1)].set(values.reshape(-1).astype(jnp.int32))


def all_plans(stream):
    return jax.vmap(replica_plan)(jax.random.split(stream, N_DP))


def drawn(stream):
    queries = jax.random.normal(jax.random.fold_in(stream, 1), (TOKENS, KVH, GROUP, HD), jnp.float32)
    keys_all = jax.random.normal(jax.random.fold_in(stream, 2), (TOKENS, KVH, HD), jnp.float32)
    queries = jnp.clip(queries, -6.0, 6.0)
    keys_all = jnp.clip(keys_all, -6.0, 6.0)
    return (queries, keys_all)


def draw_destination(key, part):
    return all_plans(jax.random.fold_in(key, 7))


def draw_group_first(key, part):
    starts = jax.random.randint(jax.random.fold_in(key, 13), (N_DP, N_CTX), 0, 8) == 0
    offset = jax.random.randint(jax.random.fold_in(key, 14), (N_DP, 1), 0, N_CTX // 2)
    places = jnp.arange(N_CTX, dtype=jnp.int32)
    inside = jnp.logical_and(places[None, :] > offset, places[None, :] < offset + N_CTX // 2)
    starts = jnp.logical_and(starts, jnp.logical_not(inside))
    starts = jnp.logical_or(starts, places[None, :] == 0)
    starts = jnp.logical_or(starts, places[None, :] == offset + N_CTX // 2)
    marked = jnp.where(starts, places[None, :], 0).astype(jnp.int32)
    return lax.cummax(marked, axis=1).astype(jnp.int32)


def draw_query_rows(key, part):
    queries, keys_all = drawn(key)
    return jnp.clip(queries, -32.0, 32.0).reshape(TOKENS, KVH * GROUP * HD).astype(jnp.bfloat16)


def draw_key_rows(key, part):
    queries, keys_all = drawn(key)
    return jnp.clip(keys_all, -8.0, 8.0).reshape(TOKENS, KVH * HD).astype(jnp.bfloat16)


def strengthened(entries, key, source, target, blocks, factor):
    owner, partner = [(jnp.arange(entries.shape[axis_at]) // (entries.shape[axis_at] // blocks)).reshape([-1 if axis == axis_at else 1 for axis in range(entries.ndim)]) for axis_at in (source, target)]
    chosen = jax.random.permutation(key, blocks)[partner]
    strong = (owner == chosen) | (owner == (partner + blocks // 2) % blocks)
    return jnp.where(strong, factor * entries, entries)


def levels(stream_key, shape, shards, least, high):
    factor_of = 1.0
    for dim, blocks in shards:
        steps = jax.random.uniform(jax.random.fold_in(jax.random.fold_in(stream_key, 6), dim), (blocks,), jnp.float32, least / len(shards), high / len(shards))
        factor_of = factor_of * jnp.repeat(jnp.exp(steps), shape[dim] // blocks).reshape((-1,) + (1,) * (len(shape) - 1 - dim))
    return factor_of


def noise(rng, shape, scale, bound, cuts=(), kind=jnp.bfloat16):
    values = jax.random.normal(rng, shape, jnp.float32) * scale
    if len(cuts) > 0:
        values = levels(rng, shape, cuts, -0.22, 0.18) * values
    return jnp.clip(values, min=-bound, max=bound).astype(kind)


def gaussian_with(key, dims, scale, bound, cuts, heavy, kind=jnp.bfloat16):
    result = scale * jax.random.normal(key, dims, jnp.float32)
    if cuts:
        result = result * levels(key, dims, cuts, -0.22, 0.18)
    return jnp.clip(strengthened(result, jax.random.fold_in(key, 3), *heavy), -bound, bound).astype(kind)


def setup_inputs(seed: int = 0) -> dict:
    arg_keys = jax.random.split(jax.random.key(seed), 7)
    return {
        "query_rows": draw_query_rows(jax.random.fold_in(arg_keys[6], 71), 0),
        "key_rows": draw_key_rows(jax.random.fold_in(arg_keys[6], 71), 0),
        "value_rows": noise(arg_keys[2], (TOKENS, KVH * HD), 1.0, 6.0, ((0, 512),)),
        "out_grad": gaussian_with(arg_keys[3], (TOKENS, KVH * GROUP * HD), 1.0, 24.0, ((0, 512),), (0, 1, 512, 6.0)),
        "destination": draw_destination(jax.random.fold_in(arg_keys[6], 71), 0),
        "group_first": draw_group_first(jax.random.fold_in(arg_keys[6], 71), 0),
    }


HIGH = lax.Precision.HIGHEST


def product(form, left, right):
    return jnp.einsum(form, left.astype(jnp.float32), right.astype(jnp.float32), precision=HIGH)


def block_attention(query_own, keys_own, values_own, grads_own, keys_prior, values_prior, linked):
    length = query_own.shape[0]
    scaling = query_own.shape[-1] ** -0.5
    places = jnp.arange(length)
    lower_mask = places[:, None] >= places[None, :]
    upper_mask = jnp.logical_and(places[:, None] >= 0 * places[None, :], linked)
    score_own = jnp.where(lower_mask, product("qhgd,khd->hgqk", query_own, keys_own) * scaling, -jnp.inf)
    score_prior = jnp.where(upper_mask, product("qhgd,khd->hgqk", query_own, keys_prior) * scaling, -jnp.inf)
    ceiling = jnp.maximum(jnp.max(score_own, axis=-1), jnp.max(score_prior, axis=-1))[..., None]
    raw_own = jnp.exp(score_own - ceiling)
    raw_prior = jnp.exp(score_prior - ceiling)
    denom = jnp.sum(raw_own, axis=-1, keepdims=True) + jnp.sum(raw_prior, axis=-1, keepdims=True)
    prob_own = raw_own / denom
    prob_prior = raw_prior / denom
    weight_own = prob_own.astype(jnp.bfloat16)
    weight_prior = prob_prior.astype(jnp.bfloat16)
    attended = (product("hgqk,khd->qhgd", weight_own, values_own)
                + product("hgqk,khd->qhgd", weight_prior, values_prior)).astype(jnp.bfloat16)
    press_own = product("qhgd,khd->hgqk", grads_own, values_own)
    press_prior = product("qhgd,khd->hgqk", grads_own, values_prior)
    centred = (jnp.sum(prob_own * press_own, axis=-1) + jnp.sum(prob_prior * press_prior, axis=-1))[..., None]
    slope_own = (prob_own * (press_own - centred) * scaling).astype(jnp.bfloat16)
    slope_prior = (prob_prior * (press_prior - centred) * scaling).astype(jnp.bfloat16)
    grad_q = (product("hgqk,khd->qhgd", slope_own, keys_own)
              + product("hgqk,khd->qhgd", slope_prior, keys_prior)).astype(jnp.bfloat16)
    key_own = product("hgqk,qhgd->khd", slope_own, query_own).astype(jnp.bfloat16)
    key_prior = product("hgqk,qhgd->khd", slope_prior, query_own).astype(jnp.bfloat16)
    value_own = product("hgqk,qhgd->khd", weight_own, grads_own).astype(jnp.bfloat16)
    value_prior = product("hgqk,qhgd->khd", weight_prior, grads_own).astype(jnp.bfloat16)
    return attended, grad_q, key_own, key_prior, value_own, value_prior


def one_block(pieces):
    return block_attention(pieces[0], pieces[1], pieces[2], pieces[3], pieces[4], pieces[5], pieces[6])


def following(parts):
    return jnp.concatenate([parts[1:], jnp.zeros_like(parts[:1])]).astype(jnp.float32)


def replica(inputs):
    queries, keys_in, values_in, grads_in, plan, firsts = inputs
    inverse = jnp.zeros_like(plan).at[plan].set(jnp.arange(RUN, dtype=jnp.int32))
    query_slots = queries[inverse].reshape(N_CTX, ROWS, KVH, GROUP, HD)
    key_slots = keys_in[inverse].reshape(N_CTX, ROWS, KVH, HD)
    value_slots = values_in[inverse].reshape(N_CTX, ROWS, KVH, HD)
    grad_slots = grads_in[inverse].reshape(N_CTX, ROWS, KVH, GROUP, HD)
    key_before = jnp.concatenate([jnp.zeros_like(key_slots[:1]), key_slots[:-1]])
    value_before = jnp.concatenate([jnp.zeros_like(value_slots[:1]), value_slots[:-1]])
    linked = firsts < jnp.arange(N_CTX, dtype=jnp.int32)
    results = lax.map(one_block, (query_slots, key_slots, value_slots, grad_slots, key_before, value_before, linked))
    attended, grad_q, key_own, key_prior, value_own, value_prior = results
    grad_k = (key_own.astype(jnp.float32) + following(key_prior)).astype(jnp.bfloat16)
    grad_v = (value_own.astype(jnp.float32) + following(value_prior)).astype(jnp.bfloat16)
    wide = KVH * GROUP * HD
    narrow = KVH * HD
    return (attended.reshape(RUN, wide)[plan], grad_q.reshape(RUN, wide)[plan],
            grad_k.reshape(RUN, narrow)[plan], grad_v.reshape(RUN, narrow)[plan])


def reference(query_rows, key_rows, value_rows, out_grad, destination, group_first):
    wide = KVH * GROUP * HD
    narrow = KVH * HD
    results = lax.map(replica, (query_rows.reshape(N_DP, RUN, wide), key_rows.reshape(N_DP, RUN, narrow),
                                value_rows.reshape(N_DP, RUN, narrow), out_grad.reshape(N_DP, RUN, wide),
                                destination, group_first))
    attended = results[0].reshape(TOKENS, wide)
    grad_query = results[1].reshape(TOKENS, wide)
    grad_key = results[2].reshape(TOKENS, narrow)
    grad_value = results[3].reshape(TOKENS, narrow)
    bias_grad = jnp.concatenate([jnp.sum(grad_query.astype(jnp.float32), axis=0),
                                 jnp.sum(grad_value.astype(jnp.float32), axis=0)]) * (TOKENS ** -0.5)
    return attended, grad_query, grad_key, grad_value, bias_grad
```

```python
import functools

import jax
import jax.numpy as jnp
from jax import lax
from jax.experimental import pallas as pl
from jax.experimental.pallas import tpu as pltpu
from jax.sharding import PartitionSpec as P

MESH = pl.DeviceIdType.MESH
VMEM = pl.BlockSpec(memory_space=pltpu.VMEM)
ANY = pl.BlockSpec(memory_space=pl.ANY)
F32 = jnp.float32
BF16 = jnp.bfloat16


def places():
    dp = lax.axis_index("dp")
    ctx = lax.axis_index("ctx")
    return dp, ctx, ctx // 16, lax.rem(ctx // 2, 8), lax.rem(ctx, 2)


def at_ctx(dp, yh, z, c):
    return (dp, yh * 16 + z * 2 + c)


def cols(start, size):
    return pl.ds(pl.multiple_of(start, 128), size)


def gather_kernel(q, k, v, g, lk, KV, QX, GX, LK, local_sem, core_send, core_recv,
                  y_send, y_recv, z_send, z_recv, l_send, l_recv):
    dp, ctx, yh, z, c = places()
    mine, other = pl.ds(c * 128, 128), 1 - c
    half = pl.ds(0, 128), pl.ds(128, 128)

    def local_pair(i, src, dst):
        copy = pltpu.make_async_copy(src, dst, local_sem.at[i])
        copy.start()
        return copy

    local = []
    for gi in range(2):
        local.append(local_pair(2 * gi, k.at[:, cols((2 * c + gi) * 128, 128)], KV.at[gi, yh, z, mine, half[0]]))
        local.append(local_pair(2 * gi + 1, v.at[:, cols((2 * c + gi) * 128, 128)], KV.at[gi, yh, z, mine, half[1]]))
    local.append(local_pair(4, q.at[:, cols(c * 2048, 2048)], QX.at[mine, :]))
    local.append(local_pair(5, g.at[:, cols(c * 2048, 2048)], GX.at[mine, :]))
    LK[ctx] = lk[0]

    barrier = pltpu.get_barrier_semaphore()
    for i in range(1, 32):
        pl.semaphore_signal(barrier, inc=1, device_id=(dp, lax.rem(ctx + i, 32)), device_id_type=MESH)
    pl.semaphore_wait(barrier, 31)

    def remote(src, dst, send, recv, device):
        copy = pltpu.make_async_remote_copy(src_ref=src, dst_ref=dst, send_sem=send, recv_sem=recv,
                                            device_id=device, device_id_type=MESH)
        copy.start()
        return copy

    pending = []
    partner = at_ctx(dp, yh, z, other)
    core = []
    for gi in range(2):
        for j, src in ((0, k), (1, v)):
            i = 2 * gi + j
            core.append(remote(src.at[:, cols((2 * other + gi) * 128, 128)], KV.at[gi, yh, z, mine, half[j]],
                               core_send.at[i], core_recv.at[i], partner))
    for i, (src, dst) in ((4, (q, QX)), (5, (g, GX))):
        core.append(remote(src.at[:, cols(other * 2048, 2048)], dst.at[mine, :],
                           core_send.at[i], core_recv.at[i], partner))

    right = at_ctx(dp, yh, lax.rem(z + 1, 8), c)
    left = at_ctx(dp, yh, lax.rem(z + 7, 8), c)
    rows = {}

    def chunk(gi, far, zz, part):
        y = 1 - yh if far else yh
        ref = KV.at[gi, y, lax.rem(zz + 8, 8)]
        return ref if part is None else ref.at[half[part], :]

    def step(gi, far, s):
        item = 2 * far + gi
        for way in range(2):
            if s > 0:
                rows[(item, way, s - 1)].wait_recv()
            part = way if s == 3 else None
            ref = chunk(gi, far, z - s if way == 0 else z + s, part)
            copy = remote(ref, ref, z_send.at[item, way, s], z_recv.at[item, way, s], right if way == 0 else left)
            rows[(item, way, s)] = copy
            pending.append(copy)

    ys = []
    for gi in range(2):
        for i in (2 * gi, 2 * gi + 1):
            local[i].wait()
            core[i].wait_recv()
        step(gi, 0, 0)
        ref = KV.at[gi, yh, z]
        ys.append(remote(ref, ref, y_send.at[gi], y_recv.at[gi], at_ctx(dp, 1 - yh, z, c)))
    flags = []
    for i in range(1, 32):
        flags.append(remote(lk.at[0], LK.at[ctx], l_send.at[i - 1], l_recv.at[i - 1], (dp, lax.rem(ctx + i, 32))))
    for s in (1,):
        step(0, 0, s)
        step(1, 0, s)
    for gi in range(2):
        ys[gi].wait_recv()
        step(gi, 1, 0)
    for s in (1, 2):
        step(0, 0, s + 1)
        step(1, 0, s + 1)
        step(0, 1, s)
        step(1, 1, s)
    step(0, 1, 3)
    step(1, 1, 3)
    for item in range(4):
        for way in range(2):
            rows[(item, way, 3)].wait_recv()
    for copy in pending + ys + core:
        copy.wait_send()
    local[4].wait()
    local[5].wait()
    core[4].wait_recv()
    core[5].wait_recv()
    for copy in flags:
        copy.wait()


def gathered(q, k, v, g, lk):
    return pl.pallas_call(
        gather_kernel,
        out_shape=(
            jax.ShapeDtypeStruct((2, 2, 8, 256, 256), BF16),
            jax.ShapeDtypeStruct((256, 2048), BF16),
            jax.ShapeDtypeStruct((256, 2048), BF16),
            jax.ShapeDtypeStruct((32, 1, 128), jnp.int32),
        ),
        in_specs=[ANY, ANY, ANY, ANY, VMEM],
        out_specs=(VMEM, VMEM, VMEM, VMEM),
        scratch_shapes=[
            pltpu.SemaphoreType.DMA((6,)),
            pltpu.SemaphoreType.DMA((6,)),
            pltpu.SemaphoreType.DMA((6,)),
            pltpu.SemaphoreType.DMA((2,)),
            pltpu.SemaphoreType.DMA((2,)),
            pltpu.SemaphoreType.DMA((4, 2, 4)),
            pltpu.SemaphoreType.DMA((4, 2, 4)),
            pltpu.SemaphoreType.DMA((31,)),
            pltpu.SemaphoreType.DMA((31,)),
        ],
        compiler_params=pltpu.CompilerParams(collective_id=0, has_side_effects=True, vmem_limit_bytes=48 * 2**20),
        name="gather",
    )(q, k, v, g, lk)


def dot(a, b, ca, cb):
    return lax.dot_general(a, b, (((ca,), (cb,)), ((), ())), preferred_element_type=F32)


def attention_kernel(own, KV, QX, GX, LK, PR, PP, PQ, D, ATT, GQ, BV, QP, GP, OP, DQP, PAD, SLOT, DS):
    chip = own[0]
    scale = 128**-0.5

    def placing(c):
        return (PR[c] == lax.broadcasted_iota(jnp.int32, (512, 256), 0)).astype(BF16)

    mine = placing(chip)

    def spread(j, _):
        at = cols(j * 256, 256)
        QP[:, at] = dot(mine, QX[:, at], 1, 0).astype(BF16)
        GP[:, at] = dot(mine, GX[:, at], 1, 0).astype(BF16)
        return 0

    lax.fori_loop(0, 8, spread, 0)
    BV[...] = jnp.zeros_like(BV)
    SLOT[0] = jnp.zeros((128, 256), BF16)

    for gi in range(2):
        def widen(c, _):
            found = dot(placing(c), KV[gi, c // 8, lax.rem(c, 8)], 1, 0).astype(BF16)
            PAD[:, pl.ds(pl.multiple_of(c * 16, 16), 16), :] = found.reshape(32, 16, 256)
            return 0

        lax.fori_loop(0, 16, widen, 0)

        def seat(b):
            return (PP[b] == lax.broadcasted_iota(jnp.int32, (128, 256), 0) + 1).astype(BF16)

        def settle(b, _):
            SLOT[b + 1] = dot(seat(b), PAD[b], 1, 0).astype(BF16)
            return 0

        lax.fori_loop(0, 32, settle, 0)
        DS[0] = jnp.zeros((128, 256), F32)

        def block(b, _):
            keys = jnp.concatenate([SLOT[b, :, 0:128], SLOT[b + 1, :, 0:128]], axis=0)
            values = jnp.concatenate([SLOT[b, :, 128:256], SLOT[b + 1, :, 128:256]], axis=0)
            at = pl.ds(pl.multiple_of(b * 16, 16), 16)
            q = jnp.concatenate([QP[at, (gi * 8 + h) * 128:(gi * 8 + h + 1) * 128] for h in range(8)], axis=0)
            o = jnp.concatenate([GP[at, (gi * 8 + h) * 128:(gi * 8 + h + 1) * 128] for h in range(8)], axis=0)
            u = lax.broadcasted_iota(jnp.int32, (128, 128), 0)
            seen_own = u <= PQ[b]
            seen_prior = jnp.broadcast_to(LK[b] > 0, (128, 128))
            seen = jnp.concatenate([seen_prior, seen_own], axis=0)
            s = jnp.where(seen, dot(keys, q, 1, 1), -jnp.inf)
            top = jnp.max(s, axis=0, keepdims=True)
            e = jnp.exp((s - top) * scale)
            probs = e * (1.0 / jnp.sum(e, axis=0, keepdims=True))
            press = dot(values, o, 1, 1)
            both = probs * press
            centred = jnp.sum(both, axis=0, keepdims=True)
            slopes = ((both - probs * centred) * scale).astype(BF16)
            weights = probs.astype(BF16)
            att = dot(weights, values, 0, 0).astype(BF16)
            gq = dot(slopes, keys, 0, 0).astype(BF16)
            for h in range(8):
                to = slice((gi * 8 + h) * 128, (gi * 8 + h + 1) * 128)
                OP[at, to] = att[h * 16:(h + 1) * 16]
                DQP[at, to] = gq[h * 16:(h + 1) * 16]
            dk = dot(slopes, q, 1, 0)
            dv = dot(weights, o, 1, 0)
            DS[b, :, 0:128] += dk[0:128]
            DS[b, :, 128:256] += dv[0:128]
            DS[b + 1, :, 0:128] = dk[128:256]
            DS[b + 1, :, 128:256] = dv[128:256]
            return 0

        lax.fori_loop(0, 32, block, 0)

        def unseat(b, total):
            grads = DS[b + 1]
            PAD[b] = dot(seat(b), grads.astype(BF16), 0, 0).astype(BF16)
            return total + jnp.sum(grads[:, 128:256].reshape(16, 8, 128), axis=0)

        total = lax.fori_loop(0, 32, unseat, jnp.zeros((8, 128), F32))
        BV[16 + gi:17 + gi, :] = jnp.sum(total, axis=0, keepdims=True)

        def narrow(c, _):
            rows = PAD[:, pl.ds(pl.multiple_of(c * 16, 16), 16), :].reshape(512, 256)
            D[gi, c // 8, lax.rem(c, 8)] = dot(placing(c), rows, 0, 0).astype(BF16)
            return 0

        lax.fori_loop(0, 16, narrow, 0)

    for j in range(8):
        at = slice(j * 256, (j + 1) * 256)
        ATT[:, at] = dot(mine, OP[:, at], 0, 0).astype(BF16)
        rows = dot(mine, DQP[:, at], 0, 0)
        GQ[:, at] = rows.astype(BF16)
        sums = jnp.sum(rows, axis=0, keepdims=True)
        BV[2 * j:2 * j + 1, :] = sums[:, 0:128]
        BV[2 * j + 1:2 * j + 2, :] = sums[:, 128:256]


def attended(own, KV, QX, GX, LK, PR, PP, PQ):
    return pl.pallas_call(
        attention_kernel,
        out_shape=(
            jax.ShapeDtypeStruct((2, 2, 8, 256, 256), BF16),
            jax.ShapeDtypeStruct((256, 2048), BF16),
            jax.ShapeDtypeStruct((256, 2048), BF16),
            jax.ShapeDtypeStruct((24, 128), F32),
        ),
        in_specs=[pl.BlockSpec(memory_space=pltpu.SMEM)] + [VMEM] * 7,
        out_specs=(VMEM,) * 4,
        scratch_shapes=[
            pltpu.VMEM((512, 2048), BF16),
            pltpu.VMEM((512, 2048), BF16),
            pltpu.VMEM((512, 2048), BF16),
            pltpu.VMEM((512, 2048), BF16),
            pltpu.VMEM((32, 256, 256), BF16),
            pltpu.VMEM((33, 128, 256), BF16),
            pltpu.VMEM((33, 128, 256), F32),
        ],
        compiler_params=pltpu.CompilerParams(vmem_limit_bytes=58 * 2**20),
        name="attend",
    )(own, KV, QX, GX, LK, PR, PP, PQ)


def reduce_kernel(D, ATT, GQ, BV, att, gq, gk, gv, BT, R, YS, YR, KS, KR, BZ, BY, BX, BM,
                  local_sem, core_send, core_recv, k_send, k_recv, y_send, y_recv, z_send, z_recv,
                  b_send, b_recv):
    dp, ctx, yh, z, c = places()
    yl, x = dp // 4, lax.rem(dp, 4)
    y = yh * 4 + yl
    other = 1 - c
    half = pl.ds(0, 128), pl.ds(128, 128)

    def at_y(yy):
        return ((lax.rem(yy, 4)) * 4 + x, (yy // 4) * 16 + z * 2 + c)

    partner = at_ctx(dp, yh, z, other)
    along_z = [(lax.rem(z + i, 8), at_ctx(dp, yh, lax.rem(z + i, 8), c)) for i in range(1, 8)]
    along_y = [(lax.rem(y + i, 8), at_y(lax.rem(y + i, 8))) for i in range(1, 8)]
    along_x = [(lax.rem(x + i, 4), (yl * 4 + lax.rem(x + i, 4), ctx)) for i in range(1, 4)]
    barrier = pltpu.get_barrier_semaphore()
    for _, device in along_z + along_y + along_x + [(0, partner)]:
        pl.semaphore_signal(barrier, inc=1, device_id=device, device_id_type=MESH)
    pl.semaphore_wait(barrier, 18)

    def remote(src, dst, send, recv, device):
        copy = pltpu.make_async_remote_copy(src_ref=src, dst_ref=dst, send_sem=send, recv_sem=recv,
                                            device_id=device, device_id_type=MESH)
        copy.start()
        return copy

    sent = []
    rows = {}
    right, left = along_z[0][1], along_z[6][1]

    def side(far):
        return 1 - yh if far else yh

    def own(gi, far, zz):
        return D.at[gi, side(far), lax.rem(zz + 8, 8)]

    def step(gi, far, s):
        item = 2 * far + gi
        for way in range(2):
            device = right if way == 0 else left
            target = z + 4 - s if way == 0 else z - 4 + s
            dst = R.at[item, way, s]
            if s == 0:
                src = own(gi, far, target).at[half[way], :]
                dst = dst.at[half[way], :]
            else:
                rows[(item, way, s - 1)].wait_recv()
                src = R.at[item, way, s - 1]
                term = own(gi, far, target)
                for part in range(2):
                    at = slice(part * 128, part * 128 + 128)
                    if s == 1 and part != way:
                        src[at, :] = term[at, :]
                    else:
                        src[at, :] = (src[at, :].astype(F32) + term[at, :].astype(F32)).astype(BF16)
            copy = remote(src, dst, z_send.at[item, way, s], z_recv.at[item, way, s], device)
            rows[(item, way, s)] = copy
            sent.append(copy)

    def total(gi, far, at):
        item = 2 * far + gi
        return (D[gi, side(far), z, at, :].astype(F32) + R[item, 0, 3, at, :].astype(F32)
                + R[item, 1, 3, at, :].astype(F32))

    step(0, 1, 0)
    step(1, 1, 0)
    step(0, 0, 0)
    step(1, 0, 0)

    def spread(buffer, place, line, base, value):
        buffer[place] = value
        out = []
        for i, (_, device) in enumerate(line):
            out.append(remote(buffer.at[place], buffer.at[place], b_send.at[base + i], b_recv.at[base + i], device))
        return out

    def summed(buffer, copies, count):
        for copy in copies:
            copy.wait_recv()
        value = buffer[0]
        for i in range(1, count):
            value = value + buffer[i]
        return value

    copies_z = spread(BZ, z, along_z, 0, BV[...])
    local = []
    core = []
    for i, (src, dst) in enumerate(((ATT, att), (GQ, gq))):
        copy = pltpu.make_async_copy(src.at[pl.ds(c * 128, 128), :], dst.at[:, cols(c * 2048, 2048)], local_sem.at[i])
        copy.start()
        local.append(copy)
        core.append(remote(src.at[pl.ds(other * 128, 128), :], dst.at[:, cols(c * 2048, 2048)],
                           core_send.at[i], core_recv.at[i], partner))

    step(0, 1, 1)
    step(1, 1, 1)
    copies_y = spread(BY, y, along_y, 7, summed(BZ, copies_z, 8))
    step(0, 1, 2)
    step(1, 1, 2)
    step(0, 0, 1)
    step(1, 0, 1)
    copies_x = spread(BX, x, along_x, 14, summed(BY, copies_y, 8))
    step(0, 1, 3)
    step(1, 1, 3)
    step(0, 0, 2)
    step(1, 0, 2)
    BM[...] = summed(BX, copies_x, 4) * (65536.0**-0.5)
    BT[c] = BM[...]
    copies_m = [remote(BM, BT.at[c], b_send.at[17], b_recv.at[17], partner)]
    ys = []
    for gi in range(2):
        rows[(2 + gi, 0, 3)].wait_recv()
        rows[(2 + gi, 1, 3)].wait_recv()
        YS[gi] = total(gi, 1, slice(0, 256)).astype(BF16)
        ys.append(remote(YS.at[gi], YR.at[gi], y_send.at[gi], y_recv.at[gi], at_ctx(dp, 1 - yh, z, c)))
    step(0, 0, 3)
    step(1, 0, 3)
    ks = []
    for gi in range(2):
        rows[(gi, 0, 3)].wait_recv()
        rows[(gi, 1, 3)].wait_recv()
        ys[gi].wait_recv()
        at = pl.ds(pl.multiple_of(other * 128, 128), 128)
        KS[gi] = (total(gi, 0, at) + YR[gi, at, :].astype(F32)).astype(BF16)
        ks.append(remote(KS.at[gi], KR.at[gi], k_send.at[gi], k_recv.at[gi], partner))
        at = pl.ds(pl.multiple_of(c * 128, 128), 128)
        done = (total(gi, 0, at) + YR[gi, at, :].astype(F32)).astype(BF16)
        gk[:, cols((2 * c + gi) * 128, 128)] = done[:, 0:128]
        gv[:, cols((2 * c + gi) * 128, 128)] = done[:, 128:256]
    for gi in range(2):
        ks[gi].wait_recv()
        gk[:, cols((2 * other + gi) * 128, 128)] = KR[gi, :, 0:128]
        gv[:, cols((2 * other + gi) * 128, 128)] = KR[gi, :, 128:256]
    copies_m[0].wait_recv()
    for copy in sent + ys + ks + copies_z + copies_y + copies_x + copies_m + core:
        copy.wait_send()
    for copy in core:
        copy.wait_recv()
    for copy in local:
        copy.wait()


def reduced(D, ATT, GQ, BV):
    dma = pltpu.SemaphoreType.DMA
    return pl.pallas_call(
        reduce_kernel,
        out_shape=(
            jax.ShapeDtypeStruct((128, 4096), BF16),
            jax.ShapeDtypeStruct((128, 4096), BF16),
            jax.ShapeDtypeStruct((128, 512), BF16),
            jax.ShapeDtypeStruct((128, 512), BF16),
            jax.ShapeDtypeStruct((2, 24, 128), F32),
        ),
        in_specs=[VMEM] * 4,
        out_specs=(ANY, ANY, VMEM, VMEM, VMEM),
        scratch_shapes=[
            pltpu.VMEM((4, 2, 4, 256, 256), BF16),
            pltpu.VMEM((2, 256, 256), BF16),
            pltpu.VMEM((2, 256, 256), BF16),
            pltpu.VMEM((2, 128, 256), BF16),
            pltpu.VMEM((2, 128, 256), BF16),
            pltpu.VMEM((8, 24, 128), F32),
            pltpu.VMEM((8, 24, 128), F32),
            pltpu.VMEM((4, 24, 128), F32),
            pltpu.VMEM((24, 128), F32),
            dma((2,)), dma((2,)), dma((2,)), dma((2,)), dma((2,)), dma((2,)), dma((2,)),
            dma((4, 2, 4)), dma((4, 2, 4)), dma((18,)), dma((18,)),
        ],
        compiler_params=pltpu.CompilerParams(collective_id=1, has_side_effects=True, vmem_limit_bytes=48 * 2**20),
        name="reduce",
    )(D, ATT, GQ, BV)


def local(query_rows, key_rows, value_rows, out_grad, destination, group_first):
    ctx = lax.axis_index("ctx")
    linked = (group_first[0, 0] < ctx).astype(jnp.int32)
    lk = jnp.broadcast_to(linked, (1, 1, 128))
    plan = destination.reshape(32, 128)
    blocks = plan // 128
    spots = plan % 128
    ids = jnp.arange(128)
    same = (blocks[:, :, None] == blocks[:, None, :]) & (ids[None, :, None] < ids[None, None, :])
    ranks = jnp.sum(same.astype(jnp.int32), axis=1)
    code = blocks * 8 + ranks
    hits = code[:, :, None] == jnp.arange(256)[None, None, :]
    PP = jnp.sum(jnp.where(hits, spots[:, :, None] + 1, 0), axis=1)
    PP = PP.reshape(32, 32, 8).transpose(1, 0, 2).reshape(32, 1, 256)
    cores = (jnp.arange(32) % 2)[:, None] * 8
    PR = (blocks * 16 + cores + ranks).reshape(16, 1, 256)
    chip = ctx // 2
    mine = lax.dynamic_slice_in_dim(PP.reshape(32, 16, 16), chip, 1, 1)
    PQ = jnp.broadcast_to(jnp.where(mine == 0, 127, mine - 1), (32, 8, 16)).reshape(32, 1, 128)
    KV, QX, GX, LK = gathered(query_rows, key_rows, value_rows, out_grad, lk)
    D, ATT, GQ, BV = attended(chip.reshape(1).astype(jnp.int32), KV, QX, GX, LK, PR, PP, PQ)
    att, gq, gk, gv, BT = reduced(D, ATT, GQ, BV)
    bias = jnp.concatenate([BT[:, :16].reshape(4096), BT[:, 16:18].reshape(512)])
    return att, gq, gk, gv, bias


def solution(mesh):
    rows = P(("dp", "ctx"), None)
    return jax.shard_map(
        local, mesh=mesh, in_specs=(rows, rows, rows, rows, P("dp", None), P("dp", "ctx")),
        out_specs=(rows, rows, rows, rows, P()), check_vma=False)
```

```python
import jax
import jax.numpy as jnp
from jax import lax
from jax.experimental import pallas as pl
from jax.experimental.pallas import tpu as pltpu
from jax.sharding import PartitionSpec as P

MESH = pl.DeviceIdType.MESH
VMEM = pl.BlockSpec(memory_space=pltpu.VMEM)
ANY = pl.BlockSpec(memory_space=pl.ANY)
F32 = jnp.float32
BF16 = jnp.bfloat16


def places():
    dp = lax.axis_index("dp")
    ctx = lax.axis_index("ctx")
    return dp, ctx, ctx // 16, lax.rem(ctx // 2, 8), lax.rem(ctx, 2)


def at_ctx(dp, yh, z, c):
    return (dp, yh * 16 + z * 2 + c)


def cols(start, size):
    return pl.ds(pl.multiple_of(start, 128), size)


SCALE = 128**-0.5
LOG2E = 1.4426950408889634
GROUPS = 4


def dot(a, b, ca, cb):
    return lax.dot_general(a, b, (((ca,), (cb,)), ((), ())), preferred_element_type=F32)


def step_kernel(q, k, v, g, lk, PR, PP, PQ, att, gq, gk, gv, BT,
                KV, QX, GX, LK, QP, GP, OP, DQP, PAD, D, ATT, GQ, BV, R, YS, YR, KS, KR, BZ, BY, BX, BM,
                local_sem, core_send, core_recv, y_send, y_recv, z_send, z_recv, l_send, l_recv,
                out_sem, o_send, o_recv, k_send, k_recv, v_send, v_recv, r_send, r_recv, b_send, b_recv):
    dp, ctx, yh, z, c = places()
    yl, x = dp // 4, lax.rem(dp, 4)
    y = yh * 4 + yl
    other = 1 - c
    half = pl.ds(0, 128), pl.ds(128, 128)
    mine = pl.ds(pl.multiple_of(c * 128, 128), 128)
    theirs = pl.ds(pl.multiple_of(other * 128, 128), 128)
    chip = yh * 8 + z

    def copied(src, dst, sem):
        copy = pltpu.make_async_copy(src, dst, sem)
        copy.start()
        return copy

    local = []
    for gi in range(2):
        at = cols((2 * c + gi) * 128, 128)
        local.append(copied(k.at[:, at], KV.at[gi, yh, z, mine, half[0]], local_sem.at[2 * gi]))
        local.append(copied(v.at[:, at], KV.at[gi, yh, z, mine, half[1]], local_sem.at[2 * gi + 1]))
    local.append(copied(q.at[:, cols(c * 2048, 2048)], QX.at[mine, :], local_sem.at[4]))
    local.append(copied(g.at[:, cols(c * 2048, 2048)], GX.at[mine, :], local_sem.at[5]))
    LK[ctx] = lk[0]

    def at_y(yy):
        return (lax.rem(yy, 4) * 4 + x, (yy // 4) * 16 + z * 2 + c)

    partner = at_ctx(dp, yh, z, other)
    across = at_ctx(dp, 1 - yh, z, c)
    peers = [(dp, lax.rem(ctx + i, 32)) for i in range(1, 32)]
    along_z = [at_ctx(dp, yh, lax.rem(z + i, 8), c) for i in range(1, 8)]
    along_y = [at_y(lax.rem(y + i, 8)) for i in range(1, 8)]
    along_x = [(yl * 4 + lax.rem(x + i, 4), ctx) for i in range(1, 4)]
    right, left = along_z[0], along_z[6]
    barrier = pltpu.get_barrier_semaphore()
    for device in peers + along_y[:3] + along_y[4:] + along_x:
        pl.semaphore_signal(barrier, inc=1, device_id=device, device_id_type=MESH)
    pl.semaphore_wait(barrier, 40)

    sent = []

    def remote(src, dst, send, recv, device):
        copy = pltpu.make_async_remote_copy(src_ref=src, dst_ref=dst, send_sem=send, recv_sem=recv,
                                            device_id=device, device_id_type=MESH)
        copy.start()
        sent.append(copy)
        return copy

    core = []
    for gi in range(2):
        at = cols((2 * other + gi) * 128, 128)
        for j, src in ((0, k), (1, v)):
            i = 2 * gi + j
            core.append(remote(src.at[:, at], KV.at[gi, yh, z, mine, half[j]], core_send.at[i], core_recv.at[i], partner))
    for i, (src, dst) in ((4, (q, QX)), (5, (g, GX))):
        core.append(remote(src.at[:, cols(other * 2048, 2048)], dst.at[mine, :], core_send.at[i], core_recv.at[i],
                           partner))

    def side(far):
        return 1 - yh if far else yh

    def ring(zz):
        return lax.rem(zz + 8, 8)

    def placing(c):
        return (PR[c] == lax.broadcasted_iota(jnp.int32, (512, 256), 0)).astype(BF16)

    def widen(gi, far, zs):
        found = [dot(placing(side(far) * 8 + zz), KV[gi, side(far), zz], 1, 0).astype(BF16) for zz in zs]
        for zz, rows in zip(zs, found):
            at = pl.ds(pl.multiple_of((side(far) * 8 + zz) * 16, 16), 16)
            PAD[gi, 1:33, at, :] = rows.reshape(32, 16, 256)

    rows = {}
    ys = {}

    def bring(gi, far, s):
        item = 2 * far + gi
        if s == 0:
            if far:
                ys[gi].wait_recv()
            else:
                for i in (2 * gi, 2 * gi + 1):
                    local[i].wait()
                    core[i].wait_recv()
        for way in range(2):
            if s > 0:
                rows[(item, way, s - 1)].wait_recv()
            if s < 4:
                ref = KV.at[gi, side(far), ring(z - s if way == 0 else z + s)]
                if s == 3:
                    ref = ref.at[half[way], :]
                rows[(item, way, s)] = remote(ref, ref, z_send.at[item, way, s], z_recv.at[item, way, s],
                                              right if way == 0 else left)
        if s == 0 and not far:
            ref = KV.at[gi, yh, z]
            ys[gi] = remote(ref, ref, y_send.at[gi], y_recv.at[gi], across)
        widen(gi, far, [ring(z + s)] if s in (0, 4) else [ring(z - s), ring(z + s)])

    def queries(ref, gi, b):
        at = slice(b * 16 + 16, b * 16 + 32)
        return jnp.concatenate([ref[at, (gi * 8 + h) * 128:(gi * 8 + h + 1) * 128] for h in range(8)], axis=0)

    def seat(b):
        return (PP[b] == lax.broadcasted_iota(jnp.int32, (128, 256), 0) + 1).astype(BF16)

    def unseat(gi, dk, dv, b):
        grads = [jnp.concatenate([dk[j], dv[j]], axis=1).astype(BF16) for j in range(len(b))]
        back = [dot(seat(b[j]), grads[j], 0, 0).astype(BF16) for j in range(len(b))]
        for j in range(len(b)):
            PAD[gi, b[j] + 1] = back[j]

    def blocks(gi, i, carry):
        s_last, p_last, w_last, sl_last, kv_last, total = carry
        un = 32 // GROUPS
        span = range(un)
        b = [i * un + j for j in span]
        kv = [dot(seat(b[j]), PAD[gi, b[j] + 1], 1, 0).astype(BF16) for j in span]
        qs = [queries(QP, gi, b[0] + j - 1) for j in range(un + 2)]
        os = [queries(GP, gi, b[0] + j - 1) for j in range(un + 2)]
        s = [dot(kv[j][:, 0:128], jnp.concatenate([qs[j + 1], qs[j + 2]], axis=0), 1, 1) for j in span]
        p = [dot(kv[j][:, 128:256], jnp.concatenate([os[j + 1], os[j + 2]], axis=0), 1, 1) for j in span]
        u = lax.broadcasted_iota(jnp.int32, (128, 128), 0)
        s_own = [jnp.where(u <= PQ[b[j]], s[j][:, 0:128], -jnp.inf) for j in span]
        s_pri = [jnp.where(jnp.broadcast_to(LK[b[j]] > 0, (128, 128)), s[j - 1][:, 128:256] if j else s_last, -jnp.inf)
                 for j in span]
        p_own = [p[j][:, 0:128] for j in span]
        p_pri = [p[j - 1][:, 128:256] if j else p_last for j in span]
        top = [jnp.max(jnp.maximum(s_own[j], s_pri[j]), axis=0, keepdims=True) for j in span]
        e_own = [jnp.exp2((s_own[j] - top[j]) * (SCALE * LOG2E)) for j in span]
        e_pri = [jnp.exp2((s_pri[j] - top[j]) * (SCALE * LOG2E)) for j in span]
        inv = [1.0 / jnp.sum(e_own[j] + e_pri[j], axis=0, keepdims=True) for j in span]
        w_own = [e_own[j] * inv[j] for j in span]
        w_pri = [e_pri[j] * inv[j] for j in span]
        centred = [jnp.sum(w_own[j] * p_own[j] + w_pri[j] * p_pri[j], axis=0, keepdims=True) for j in span]
        sl_own = [((w_own[j] * (p_own[j] - centred[j])) * SCALE).astype(BF16) for j in span]
        sl_pri = [((w_pri[j] * (p_pri[j] - centred[j])) * SCALE).astype(BF16) for j in span]
        w_own = [w.astype(BF16) for w in w_own]
        w_pri = [w.astype(BF16) for w in w_pri]
        att, gq, dk, dv = [], [], [], []
        for j in span:
            pair = jnp.concatenate([kv[j - 1] if j else kv_last, kv[j]], axis=0)
            att.append(dot(jnp.concatenate([w_pri[j], w_own[j]], axis=0), pair[:, 128:256], 0, 0).astype(BF16))
            gq.append(dot(jnp.concatenate([sl_pri[j], sl_own[j]], axis=0), pair[:, 0:128], 0, 0).astype(BF16))
            dk.append(dot(jnp.concatenate([sl_own[j - 1] if j else sl_last, sl_pri[j]], axis=1),
                          jnp.concatenate([qs[j], qs[j + 1]], axis=0), 1, 0))
            dv.append(dot(jnp.concatenate([w_own[j - 1] if j else w_last, w_pri[j]], axis=1),
                          jnp.concatenate([os[j], os[j + 1]], axis=0), 1, 0))
        for j in span:
            at = slice(b[j] * 16, b[j] * 16 + 16)
            for h in range(8):
                to = slice((gi * 8 + h) * 128, (gi * 8 + h + 1) * 128)
                OP[at, to] = att[j][h * 16:(h + 1) * 16]
                DQP[at, to] = gq[j][h * 16:(h + 1) * 16]
        first = 0 if i else 1
        unseat(gi, dk[first:], dv[first:], [bj - 1 for bj in b[first:]])
        for j in span[first:]:
            total = total + jnp.sum(dv[j].reshape(16, 8, 128), axis=0)
        if i == GROUPS - 1:
            dk = dot(sl_own[-1], qs[un], 1, 0)
            dv = dot(w_own[-1], os[un], 1, 0)
            unseat(gi, [dk], [dv], [31])
            total = total + jnp.sum(dv.reshape(16, 8, 128), axis=0)
            BV[16 + gi:17 + gi, :] = jnp.sum(total, axis=0, keepdims=True)
        return s[-1][:, 128:256], p[-1][:, 128:256], w_own[-1], sl_own[-1], kv[-1], total

    def opening():
        zf = jnp.zeros((128, 128), F32)
        zb = jnp.zeros((128, 128), BF16)
        return zf, zf, zb, zb, jnp.zeros((128, 256), BF16), jnp.zeros((8, 128), F32)

    def narrow(gi, places):
        out = []
        for far, zz in places:
            at = pl.ds(pl.multiple_of((side(far) * 8 + zz) * 16, 16), 16)
            wide = PAD[gi, 1:33, at, :].reshape(512, 256)
            out.append(dot(placing(side(far) * 8 + zz), wide, 0, 0).astype(BF16))
        for (far, zz), value in zip(places, out):
            D[gi, side(far), zz] = value

    back = {}

    def give(gi, far, s):
        item = 2 * far + gi
        for way in range(2):
            target = z + 4 - s if way == 0 else z - 4 + s
            term = D.at[gi, side(far), ring(target)]
            dst = R.at[item, way, s]
            if s == 0:
                src = term.at[half[way], :]
                dst = dst.at[half[way], :]
            else:
                back[(item, way, s - 1)].wait_recv()
                src = R.at[item, way, s - 1]
                for part in range(2):
                    at = slice(part * 128, part * 128 + 128)
                    if s == 1 and part != way:
                        src[at, :] = term[at, :]
                    else:
                        src[at, :] = (src[at, :].astype(F32) + term[at, :].astype(F32)).astype(BF16)
            back[(item, way, s)] = remote(src, dst, r_send.at[item, way, s], r_recv.at[item, way, s],
                                          right if way == 0 else left)

    def total(gi, far, at):
        item = 2 * far + gi
        return (D[gi, side(far), z, at, :].astype(F32) + R[item, 0, 3, at, :].astype(F32)
                + R[item, 1, 3, at, :].astype(F32))

    def finish(gi, far):
        item = 2 * far + gi
        back[(item, 0, 3)].wait_recv()
        back[(item, 1, 3)].wait_recv()
        if far:
            YS[gi] = total(gi, 1, slice(0, 256)).astype(BF16)
            ys[gi] = remote(YS.at[gi], YR.at[gi], v_send.at[gi], v_recv.at[gi], across)
            return
        ys[gi].wait_recv()
        KS[gi] = (total(gi, 0, theirs) + YR[gi, theirs, :].astype(F32)).astype(BF16)
        ks.append(remote(KS.at[gi], KR.at[gi], k_send.at[gi], k_recv.at[gi], partner))
        done = (total(gi, 0, mine) + YR[gi, mine, :].astype(F32)).astype(BF16)
        gk[:, cols((2 * c + gi) * 128, 128)] = done[:, 0:128]
        gv[:, cols((2 * c + gi) * 128, 128)] = done[:, 128:256]

    def start_reduce(gi):
        narrow(gi, [(1, ring(z + 4)), (0, ring(z + 4))])
        give(gi, 1, 0)
        give(gi, 0, 0)
        narrow(gi, [(far, ring(z + i)) for i in (3, 5) for far in (1, 0)])
        narrow(gi, [(far, ring(z + i)) for i in (2, 6) for far in (1, 0)])
        narrow(gi, [(far, ring(z + i)) for i in (1, 7) for far in (1, 0)])
        narrow(gi, [(far, z) for far in (1, 0)])

    ks = []
    BV[...] = jnp.zeros_like(BV)
    zeros = jnp.zeros((16, 2048), BF16)
    for ref in (QP, GP):
        ref[0:16, :] = zeros
        ref[528:544, :] = zeros

    bring(0, 0, 0)
    bring(1, 0, 0)
    flags = [remote(lk.at[0], LK.at[ctx], l_send.at[i], l_recv.at[i], peers[i]) for i in range(31)]
    for i in (4, 5):
        local[i].wait()
        core[i].wait_recv()
    here = placing(chip)

    def spread(ref, src, j):
        at = slice(j * 256, (j + 1) * 256)
        ref[16:528, at] = dot(here, src[:, at], 1, 0).astype(BF16)

    for j in range(4):
        spread(QP, QX, j)
    bring(0, 0, 1)
    for j in range(4):
        spread(GP, GX, j)
    bring(0, 1, 0)
    for j in range(4, 8):
        spread(QP, QX, j)
    bring(0, 0, 2)
    for j in range(4, 8):
        spread(GP, GX, j)
    bring(0, 1, 1)
    bring(0, 0, 3)
    bring(0, 1, 2)
    bring(0, 0, 4)
    bring(1, 0, 1)
    bring(0, 1, 3)
    bring(1, 1, 0)
    for copy in flags:
        copy.wait_recv()
    bring(0, 1, 4)

    carry = blocks(0, 0, opening())
    bring(1, 0, 2)
    bring(1, 1, 1)
    carry = blocks(0, 1, carry)
    bring(1, 0, 3)
    carry = blocks(0, 2, carry)
    bring(1, 1, 2)
    carry = blocks(0, 3, carry)
    bring(1, 0, 4)
    start_reduce(0)
    bring(1, 1, 3)
    give(0, 1, 1)
    bring(1, 1, 4)
    carry = blocks(1, 0, opening())
    give(0, 0, 1)
    carry = blocks(1, 1, carry)
    give(0, 1, 2)
    carry = blocks(1, 2, carry)
    give(0, 0, 2)
    carry = blocks(1, 3, carry)
    start_reduce(1)
    give(0, 1, 3)
    here = placing(chip)
    for j in range(8):
        at = slice(j * 256, (j + 1) * 256)
        ATT[:, at] = dot(here, OP[:, at], 0, 0).astype(BF16)
        wide = dot(here, DQP[:, at], 0, 0)
        GQ[:, at] = wide.astype(BF16)
        sums = jnp.sum(wide, axis=0, keepdims=True)
        BV[2 * j:2 * j + 1, :] = sums[:, 0:128]
        BV[2 * j + 1:2 * j + 2, :] = sums[:, 128:256]
    give(0, 0, 3)
    outs = []
    for i, (src, dst) in enumerate(((ATT, att), (GQ, gq))):
        outs.append(copied(src.at[mine, :], dst.at[:, cols(c * 2048, 2048)], out_sem.at[i]))
        core.append(remote(src.at[theirs, :], dst.at[:, cols(c * 2048, 2048)], o_send.at[i], o_recv.at[i], partner))

    def share(buffer, place, line, base, value):
        buffer[place] = value
        return [remote(buffer.at[place], buffer.at[place], b_send.at[base + i], b_recv.at[base + i], device)
                for i, device in enumerate(line)]

    def summed(buffer, copies, count):
        for copy in copies:
            copy.wait_recv()
        value = buffer[0]
        for i in range(1, count):
            value = value + buffer[i]
        return value

    copies = share(BZ, z, along_z, 0, BV[...])
    give(1, 1, 1)
    finish(0, 1)
    copies = share(BY, y, along_y, 7, summed(BZ, copies, 8))
    give(1, 0, 1)
    give(1, 1, 2)
    copies = share(BX, x, along_x, 14, summed(BY, copies, 8))
    finish(0, 0)
    give(1, 0, 2)
    give(1, 1, 3)
    BM[...] = summed(BX, copies, 4) * (65536.0**-0.5)
    BT[c] = BM[...]
    last = remote(BM, BT.at[c], b_send.at[17], b_recv.at[17], partner)
    give(1, 0, 3)
    finish(1, 1)
    finish(1, 0)
    for gi in range(2):
        ks[gi].wait_recv()
        gk[:, cols((2 * other + gi) * 128, 128)] = KR[gi, :, 0:128]
        gv[:, cols((2 * other + gi) * 128, 128)] = KR[gi, :, 128:256]
    last.wait_recv()
    for copy in core[6:]:
        copy.wait_recv()
    for copy in outs:
        copy.wait()
    for copy in sent:
        copy.wait_send()


def stepped(q, k, v, g, lk, PR, PP, PQ):
    dma = pltpu.SemaphoreType.DMA
    return pl.pallas_call(
        step_kernel,
        out_shape=(
            jax.ShapeDtypeStruct((128, 4096), BF16),
            jax.ShapeDtypeStruct((128, 4096), BF16),
            jax.ShapeDtypeStruct((128, 512), BF16),
            jax.ShapeDtypeStruct((128, 512), BF16),
            jax.ShapeDtypeStruct((2, 24, 128), F32),
        ),
        in_specs=[ANY] * 4 + [VMEM] * 4,
        out_specs=(ANY, ANY, VMEM, VMEM, VMEM),
        scratch_shapes=[
            pltpu.VMEM((2, 2, 8, 256, 256), BF16),
            pltpu.VMEM((256, 2048), BF16),
            pltpu.VMEM((256, 2048), BF16),
            pltpu.VMEM((32, 1, 128), jnp.int32),
            pltpu.VMEM((544, 2048), BF16),
            pltpu.VMEM((544, 2048), BF16),
            pltpu.VMEM((512, 2048), BF16),
            pltpu.VMEM((512, 2048), BF16),
            pltpu.VMEM((2, 33, 256, 256), BF16),
            pltpu.VMEM((2, 2, 8, 256, 256), BF16),
            pltpu.VMEM((256, 2048), BF16),
            pltpu.VMEM((256, 2048), BF16),
            pltpu.VMEM((24, 128), F32),
            pltpu.VMEM((4, 2, 4, 256, 256), BF16),
            pltpu.VMEM((2, 256, 256), BF16),
            pltpu.VMEM((2, 256, 256), BF16),
            pltpu.VMEM((2, 128, 256), BF16),
            pltpu.VMEM((2, 128, 256), BF16),
            pltpu.VMEM((8, 24, 128), F32),
            pltpu.VMEM((8, 24, 128), F32),
            pltpu.VMEM((4, 24, 128), F32),
            pltpu.VMEM((24, 128), F32),
            dma((6,)), dma((6,)), dma((6,)), dma((2,)), dma((2,)), dma((4, 2, 4)), dma((4, 2, 4)), dma((31,)), dma((31,)),
            dma((2,)), dma((2,)), dma((2,)), dma((2,)), dma((2,)), dma((2,)), dma((2,)), dma((4, 2, 4)), dma((4, 2, 4)),
            dma((18,)), dma((18,)),
        ],
        compiler_params=pltpu.CompilerParams(collective_id=0, has_side_effects=True, vmem_limit_bytes=62 * 2**20),
        name="step",
    )(q, k, v, g, lk, PR, PP, PQ)


def local(query_rows, key_rows, value_rows, out_grad, destination, group_first):
    ctx = lax.axis_index("ctx")
    linked = (group_first[0, 0] < ctx).astype(jnp.int32)
    lk = jnp.broadcast_to(linked, (1, 1, 128))
    plan = destination.reshape(32, 128)
    blocks = plan // 128
    spots = plan % 128
    ids = jnp.arange(128)
    same = (blocks[:, :, None] == blocks[:, None, :]) & (ids[None, :, None] < ids[None, None, :])
    ranks = jnp.sum(same.astype(jnp.int32), axis=1)
    code = blocks * 8 + ranks
    hits = code[:, :, None] == jnp.arange(256)[None, None, :]
    PP = jnp.sum(jnp.where(hits, spots[:, :, None] + 1, 0), axis=1)
    PP = PP.reshape(32, 32, 8).transpose(1, 0, 2).reshape(32, 1, 256)
    cores = (jnp.arange(32) % 2)[:, None] * 8
    PR = (blocks * 16 + cores + ranks).reshape(16, 1, 256)
    chip = ctx // 2
    mine = lax.dynamic_slice_in_dim(PP.reshape(32, 16, 16), chip, 1, 1)
    PQ = jnp.broadcast_to(jnp.where(mine == 0, 127, mine - 1), (32, 8, 16)).reshape(32, 1, 128)
    att, gq, gk, gv, BT = stepped(query_rows, key_rows, value_rows, out_grad, lk, PR, PP, PQ)
    bias = jnp.concatenate([BT[:, :16].reshape(4096), BT[:, 16:18].reshape(512)])
    return att, gq, gk, gv, bias


def solution(mesh):
    rows = P(("dp", "ctx"), None)
    return jax.shard_map(
        local, mesh=mesh, in_specs=(rows, rows, rows, rows, P("dp", None), P("dp", "ctx")),
        out_specs=(rows, rows, rows, rows, P()), check_vma=False)
```

```python
import jax
import jax.numpy as jnp
from jax import lax
from jax.experimental import pallas as pl
from jax.experimental.pallas import tpu as pltpu
from jax.sharding import PartitionSpec as P

MESH = pl.DeviceIdType.MESH
VMEM = pl.BlockSpec(memory_space=pltpu.VMEM)
ANY = pl.BlockSpec(memory_space=pl.ANY)
HBM = pl.BlockSpec(memory_space=pltpu.HBM)
LIMIT = 62
F32 = jnp.float32
BF16 = jnp.bfloat16


def places():
    dp = lax.axis_index("dp")
    ctx = lax.axis_index("ctx")
    return dp, ctx, ctx // 16, lax.rem(ctx // 2, 8), lax.rem(ctx, 2)


def at_ctx(dp, yh, z, c):
    return (dp, yh * 16 + z * 2 + c)


def cols(start, size):
    return pl.ds(pl.multiple_of(start, 128), size)


SCALE = 128**-0.5
LOG2E = 1.4426950408889634
GROUPS = 4


def dot(a, b, ca, cb):
    return lax.dot_general(a, b, (((ca,), (cb,)), ((), ())), preferred_element_type=F32)


def step_kernel(q, k, v, g, plan, first, att, gq, gk, gv, bias,
                KV, QX, GX, LK, PS, PP, PQ, BT, QP, GP, OP, DQP, PAD, D, ATT, GQ, BV, R, YS, YR, KS, KR, BZ, BY, BX, BM,
                local_sem, core_send, core_recv, y_send, y_recv, z_send, z_recv, l_send, l_recv,
                out_sem, o_send, o_recv, k_send, k_recv, v_send, v_recv, r_send, r_recv, b_send, b_recv):
    dp, ctx, yh, z, c = places()
    yl, x = dp // 4, lax.rem(dp, 4)
    y = yh * 4 + yl
    other = 1 - c
    half = pl.ds(0, 128), pl.ds(128, 128)
    mine = pl.ds(pl.multiple_of(c * 128, 128), 128)
    theirs = pl.ds(pl.multiple_of(other * 128, 128), 128)
    chip = yh * 8 + z

    def copied(src, dst, sem):
        copy = pltpu.make_async_copy(src, dst, sem)
        copy.start()
        return copy

    local = []
    for gi in range(2):
        at = cols((2 * c + gi) * 128, 128)
        local.append(copied(k.at[:, at], KV.at[gi, yh, z, mine, half[0]], local_sem.at[2 * gi]))
        local.append(copied(v.at[:, at], KV.at[gi, yh, z, mine, half[1]], local_sem.at[2 * gi + 1]))
    local.append(copied(q.at[:, cols(c * 2048, 2048)], QX.at[mine, :], local_sem.at[4]))
    local.append(copied(g.at[:, cols(c * 2048, 2048)], GX.at[mine, :], local_sem.at[5]))
    flag = c * 16 + yh * 8 + z
    LK[flag] = (jnp.broadcast_to(first[...], (1, 128)) < ctx).astype(jnp.int32)

    def at_y(yy):
        return (lax.rem(yy, 4) * 4 + x, (yy // 4) * 16 + z * 2 + c)

    partner = at_ctx(dp, yh, z, other)
    across = at_ctx(dp, 1 - yh, z, c)
    along_z = [at_ctx(dp, yh, lax.rem(z + i, 8), c) for i in range(1, 8)]
    along_y = [at_y(lax.rem(y + i, 8)) for i in range(1, 8)]
    along_x = [(yl * 4 + lax.rem(x + i, 4), ctx) for i in range(1, 4)]
    right, left = along_z[0], along_z[6]
    barrier = pltpu.get_barrier_semaphore()
    for device in along_z + along_y + along_x + [partner]:
        pl.semaphore_signal(barrier, inc=1, device_id=device, device_id_type=MESH)
    pl.semaphore_wait(barrier, 18)

    sent = []

    def remote(src, dst, send, recv, device):
        copy = pltpu.make_async_remote_copy(src_ref=src, dst_ref=dst, send_sem=send, recv_sem=recv,
                                            device_id=device, device_id_type=MESH)
        copy.start()
        sent.append(copy)
        return copy

    core = []
    for gi in range(2):
        at = cols((2 * other + gi) * 128, 128)
        for j, src in ((0, k), (1, v)):
            i = 2 * gi + j
            core.append(remote(src.at[:, at], KV.at[gi, yh, z, mine, half[j]], core_send.at[i], core_recv.at[i], partner))
    for i, (src, dst) in ((4, (q, QX)), (5, (g, GX))):
        core.append(remote(src.at[:, cols(other * 2048, 2048)], dst.at[mine, :], core_send.at[i], core_recv.at[i],
                           partner))

    def side(far):
        return 1 - yh if far else yh

    def ring(zz):
        return lax.rem(zz + 8, 8)

    def placing(c):
        at = lax.broadcasted_iota(jnp.int32, (512, 128), 0)
        return jnp.concatenate([(PS[pl.ds(2 * c + i, 1), :] == at).astype(BF16) for i in range(2)], axis=1)

    def tables():
        def iota(shape, dim):
            return lax.broadcasted_iota(jnp.int32, shape, dim)

        block = plan[...] // 128
        spot = plan[...] - block * 128
        found = jnp.concatenate([block, spot + 1], axis=0).astype(F32)
        found = jnp.concatenate([found, jnp.zeros((64, 128), F32)], axis=0).T.astype(BF16)
        lane = iota((128, 1024), 1)
        device = (iota((128, 1024), 0) == lane // 32).astype(BF16)
        inside = dot(found, device, 1, 0) == (lane % 32).astype(F32)
        member = inside.astype(BF16)
        earlier = dot((iota((128, 128), 0) > iota((128, 128), 1)).astype(BF16), member, 1, 0)
        ranks = dot(jnp.where(inside, earlier, 0.0).astype(BF16), device, 1, 1)
        PS[...] = block * 16 + iota((32, 128), 0) % 2 * 8 + ranks.T[0:32].astype(jnp.int32)
        lane = iota((128, 256), 1)
        row = iota((128, 256), 0)
        rank = dot(ranks.astype(BF16), (row == lane // 8).astype(BF16), 1, 0)
        value = dot(found, (row == lane // 8 + 32).astype(BF16), 1, 0)
        filled = jnp.where(rank == (lane % 8).astype(F32), value, 0.0).astype(BF16)
        every = dot(member, filled, 0, 0)
        lane = iota((32, 256), 1) // 8
        table = jnp.zeros((32, 256), F32)
        for i in range(32):
            table = table + jnp.where(lane == i, every[i * 32:i * 32 + 32], 0.0)
        PP[...] = table.astype(jnp.int32)
        own = (iota((256, 128), 0) == chip * 16 + iota((256, 128), 1) % 16).astype(BF16)
        own = dot(table.astype(BF16), own, 1, 0).astype(jnp.int32)
        PQ[...] = jnp.where(own == 0, 127, own - 1)

    def widen(gi, far, zs):
        found = [dot(placing(side(far) * 8 + zz), KV[gi, side(far), zz], 1, 0).astype(BF16) for zz in zs]
        for zz, rows in zip(zs, found):
            at = pl.ds(pl.multiple_of((side(far) * 8 + zz) * 16, 16), 16)
            PAD[gi, 1:33, at, :] = rows.reshape(32, 16, 256)

    rows = {}
    ys = {}

    def bring(gi, far, s, later=False):
        item = 2 * far + gi
        if s == 0:
            if far:
                ys[gi].wait_recv()
            else:
                for i in (2 * gi, 2 * gi + 1):
                    local[i].wait()
                    core[i].wait_recv()
        for way in range(2):
            if s > 0:
                rows[(item, way, s - 1)].wait_recv()
            if s < 4:
                ref = KV.at[gi, side(far), ring(z - s if way == 0 else z + s)]
                if s == 3:
                    ref = ref.at[half[way], :]
                rows[(item, way, s)] = remote(ref, ref, z_send.at[item, way, s], z_recv.at[item, way, s],
                                              right if way == 0 else left)
        if s == 0 and not far:
            ref = KV.at[gi, yh, z]
            ys[gi] = remote(ref, ref, y_send.at[gi], y_recv.at[gi], across)
        if not later:
            widen(gi, far, [ring(z + s)] if s in (0, 4) else [ring(z - s), ring(z + s)])

    def queries(ref, gi, b):
        at = slice(b * 16 + 16, b * 16 + 32)
        return jnp.concatenate([ref[at, (gi * 8 + h) * 128:(gi * 8 + h + 1) * 128] for h in range(8)], axis=0)

    def seat(b):
        return (PP[b:b + 1, :] == lax.broadcasted_iota(jnp.int32, (128, 256), 0) + 1).astype(BF16)

    def unseat(gi, dk, dv, b):
        grads = [jnp.concatenate([dk[j], dv[j]], axis=1).astype(BF16) for j in range(len(b))]
        back = [dot(seat(b[j]), grads[j], 0, 0).astype(BF16) for j in range(len(b))]
        for j in range(len(b)):
            PAD[gi, b[j] + 1] = back[j]

    def blocks(gi, i, carry):
        s_last, p_last, w_last, sl_last, kv_last, total = carry
        un = 32 // GROUPS
        span = range(un)
        b = [i * un + j for j in span]
        kv = [dot(seat(b[j]), PAD[gi, b[j] + 1], 1, 0).astype(BF16) for j in span]
        qs = [queries(QP, gi, b[0] + j - 1) for j in range(un + 2)]
        os = [queries(GP, gi, b[0] + j - 1) for j in range(un + 2)]
        s = [dot(kv[j][:, 0:128], jnp.concatenate([qs[j + 1], qs[j + 2]], axis=0), 1, 1) for j in span]
        p = [dot(kv[j][:, 128:256], jnp.concatenate([os[j + 1], os[j + 2]], axis=0), 1, 1) for j in span]
        u = lax.broadcasted_iota(jnp.int32, (128, 128), 0)
        s_own = [jnp.where(u <= PQ[b[j]:b[j] + 1, :], s[j][:, 0:128], -jnp.inf) for j in span]
        s_pri = [jnp.where(jnp.broadcast_to(LK[seen_at(b[j])] > 0, (128, 128)), s[j - 1][:, 128:256] if j else s_last, -jnp.inf)
                 for j in span]
        p_own = [p[j][:, 0:128] for j in span]
        p_pri = [p[j - 1][:, 128:256] if j else p_last for j in span]
        top = [jnp.max(jnp.maximum(s_own[j], s_pri[j]), axis=0, keepdims=True) for j in span]
        e_own = [jnp.exp2((s_own[j] - top[j]) * (SCALE * LOG2E)) for j in span]
        e_pri = [jnp.exp2((s_pri[j] - top[j]) * (SCALE * LOG2E)) for j in span]
        inv = [1.0 / jnp.sum(e_own[j] + e_pri[j], axis=0, keepdims=True) for j in span]
        w_own = [e_own[j] * inv[j] for j in span]
        w_pri = [e_pri[j] * inv[j] for j in span]
        centred = [jnp.sum(w_own[j] * p_own[j] + w_pri[j] * p_pri[j], axis=0, keepdims=True) for j in span]
        sl_own = [((w_own[j] * (p_own[j] - centred[j])) * SCALE).astype(BF16) for j in span]
        sl_pri = [((w_pri[j] * (p_pri[j] - centred[j])) * SCALE).astype(BF16) for j in span]
        w_own = [w.astype(BF16) for w in w_own]
        w_pri = [w.astype(BF16) for w in w_pri]
        att, gq, dk, dv = [], [], [], []
        for j in span:
            pair = jnp.concatenate([kv[j - 1] if j else kv_last, kv[j]], axis=0)
            att.append(dot(jnp.concatenate([w_pri[j], w_own[j]], axis=0), pair[:, 128:256], 0, 0).astype(BF16))
            gq.append(dot(jnp.concatenate([sl_pri[j], sl_own[j]], axis=0), pair[:, 0:128], 0, 0).astype(BF16))
            dk.append(dot(jnp.concatenate([sl_own[j - 1] if j else sl_last, sl_pri[j]], axis=1),
                          jnp.concatenate([qs[j], qs[j + 1]], axis=0), 1, 0))
            dv.append(dot(jnp.concatenate([w_own[j - 1] if j else w_last, w_pri[j]], axis=1),
                          jnp.concatenate([os[j], os[j + 1]], axis=0), 1, 0))
        for j in span:
            at = slice(b[j] * 16, b[j] * 16 + 16)
            for h in range(8):
                to = slice((gi * 8 + h) * 128, (gi * 8 + h + 1) * 128)
                OP[at, to] = att[j][h * 16:(h + 1) * 16]
                DQP[at, to] = gq[j][h * 16:(h + 1) * 16]
        first = 0 if i else 1
        unseat(gi, dk[first:], dv[first:], [bj - 1 for bj in b[first:]])
        for j in span[first:]:
            total = total + jnp.sum(dv[j].reshape(16, 8, 128), axis=0)
        if i == GROUPS - 1:
            dk = dot(sl_own[-1], qs[un], 1, 0)
            dv = dot(w_own[-1], os[un], 1, 0)
            unseat(gi, [dk], [dv], [31])
            total = total + jnp.sum(dv.reshape(16, 8, 128), axis=0)
            BV[16 + gi:17 + gi, :] = jnp.sum(total, axis=0, keepdims=True)
        return s[-1][:, 128:256], p[-1][:, 128:256], w_own[-1], sl_own[-1], kv[-1], total

    def seen_at(b):
        return b % 2 * 16 + b // 16 * 8 + b // 2 % 8

    def opening():
        zf = jnp.zeros((128, 128), F32)
        zb = jnp.zeros((128, 128), BF16)
        return zf, zf, zb, zb, jnp.zeros((128, 256), BF16), jnp.zeros((8, 128), F32)

    def narrow(gi, places):
        out = []
        for far, zz in places:
            at = pl.ds(pl.multiple_of((side(far) * 8 + zz) * 16, 16), 16)
            wide = PAD[gi, 1:33, at, :].reshape(512, 256)
            out.append(dot(placing(side(far) * 8 + zz), wide, 0, 0).astype(BF16))
        for (far, zz), value in zip(places, out):
            D[gi, side(far), zz] = value

    back = {}

    def give(gi, far, s):
        item = 2 * far + gi
        for way in range(2):
            target = z + 4 - s if way == 0 else z - 4 + s
            term = D.at[gi, side(far), ring(target)]
            dst = R.at[item, way, s]
            if s == 0:
                src = term.at[half[way], :]
                dst = dst.at[half[way], :]
            else:
                back[(item, way, s - 1)].wait_recv()
                src = R.at[item, way, s - 1]
                for part in range(2):
                    at = slice(part * 128, part * 128 + 128)
                    if s == 1 and part != way:
                        src[at, :] = term[at, :]
                    else:
                        src[at, :] = (src[at, :].astype(F32) + term[at, :].astype(F32)).astype(BF16)
            back[(item, way, s)] = remote(src, dst, r_send.at[item, way, s], r_recv.at[item, way, s],
                                          right if way == 0 else left)

    def total(gi, far, at):
        item = 2 * far + gi
        return (D[gi, side(far), z, at, :].astype(F32) + R[item, 0, 3, at, :].astype(F32)
                + R[item, 1, 3, at, :].astype(F32))

    def finish(gi, far):
        item = 2 * far + gi
        back[(item, 0, 3)].wait_recv()
        back[(item, 1, 3)].wait_recv()
        if far:
            YS[gi] = total(gi, 1, slice(0, 256)).astype(BF16)
            ys[gi] = remote(YS.at[gi], YR.at[gi], v_send.at[gi], v_recv.at[gi], across)
            return
        ys[gi].wait_recv()
        KS[gi] = (total(gi, 0, theirs) + YR[gi, theirs, :].astype(F32)).astype(BF16)
        ks.append(remote(KS.at[gi], KR.at[gi], k_send.at[gi], k_recv.at[gi], partner))
        done = (total(gi, 0, mine) + YR[gi, mine, :].astype(F32)).astype(BF16)
        gk[:, cols((2 * c + gi) * 128, 128)] = done[:, 0:128]
        gv[:, cols((2 * c + gi) * 128, 128)] = done[:, 128:256]

    def start_reduce(gi):
        narrow(gi, [(1, ring(z + 4)), (0, ring(z + 4))])
        give(gi, 1, 0)
        give(gi, 0, 0)
        narrow(gi, [(far, ring(z + i)) for i in (3, 5) for far in (1, 0)])
        narrow(gi, [(far, ring(z + i)) for i in (2, 6) for far in (1, 0)])
        narrow(gi, [(far, ring(z + i)) for i in (1, 7) for far in (1, 0)])
        narrow(gi, [(far, z) for far in (1, 0)])

    ks = []

    bring(0, 0, 0, later=True)
    bring(1, 0, 0, later=True)
    flags = [remote(LK.at[flag], LK.at[flag], l_send.at[i], l_recv.at[i], along_z[i]) for i in range(7)]
    tables()
    BV[...] = jnp.zeros_like(BV)
    zeros = jnp.zeros((16, 2048), BF16)
    for ref in (QP, GP):
        ref[0:16, :] = zeros
        ref[528:544, :] = zeros
    for gi in range(2):
        widen(gi, 0, [z])
    for i in (4, 5):
        local[i].wait()
        core[i].wait_recv()
    here = placing(chip)

    def spread(ref, src, j):
        at = slice(j * 256, (j + 1) * 256)
        ref[16:528, at] = dot(here, src[:, at], 1, 0).astype(BF16)

    for j in range(4):
        spread(QP, QX, j)
    bring(0, 0, 1)
    for copy in flags:
        copy.wait_recv()
    part = pl.ds(c * 16 + yh * 8, 8)
    flag_y = remote(LK.at[part], LK.at[part], l_send.at[7], l_recv.at[7], across)
    for j in range(4):
        spread(GP, GX, j)
    bring(1, 0, 1)
    bring(0, 1, 0)
    for j in range(4, 8):
        spread(QP, QX, j)
    flag_y.wait_recv()
    part = pl.ds(c * 16, 16)
    flag_core = remote(LK.at[part], LK.at[part], l_send.at[8], l_recv.at[8], partner)
    bring(0, 0, 2)
    for j in range(4, 8):
        spread(GP, GX, j)
    bring(0, 1, 1)
    bring(0, 0, 3)
    bring(0, 1, 2)
    bring(1, 1, 0)
    bring(0, 1, 3)
    bring(1, 0, 2)
    flag_core.wait_recv()
    bring(0, 0, 4)
    bring(0, 1, 4)
    bring(1, 1, 1)
    carry = blocks(0, 0, opening())
    bring(1, 0, 3)
    carry = blocks(0, 1, carry)
    bring(1, 1, 2)
    carry = blocks(0, 2, carry)
    bring(1, 0, 4)
    carry = blocks(0, 3, carry)
    bring(1, 1, 3)
    start_reduce(0)
    bring(1, 1, 4)
    give(0, 1, 1)
    give(0, 0, 1)
    carry = blocks(1, 0, opening())
    give(0, 1, 2)
    carry = blocks(1, 1, carry)
    give(0, 0, 2)
    carry = blocks(1, 2, carry)
    give(0, 1, 3)
    carry = blocks(1, 3, carry)
    start_reduce(1)
    give(0, 0, 3)
    here = placing(chip)
    for j in range(8):
        at = slice(j * 256, (j + 1) * 256)
        ATT[:, at] = dot(here, OP[:, at], 0, 0).astype(BF16)
        wide = dot(here, DQP[:, at], 0, 0)
        GQ[:, at] = wide.astype(BF16)
        sums = jnp.sum(wide, axis=0, keepdims=True)
        BV[2 * j:2 * j + 1, :] = sums[:, 0:128]
        BV[2 * j + 1:2 * j + 2, :] = sums[:, 128:256]
    give(1, 1, 1)
    outs = []
    for i, (src, dst) in enumerate(((ATT, att), (GQ, gq))):
        outs.append(copied(src.at[mine, :], dst.at[:, cols(c * 2048, 2048)], out_sem.at[i]))
        core.append(remote(src.at[theirs, :], dst.at[:, cols(c * 2048, 2048)], o_send.at[i], o_recv.at[i], partner))

    def share(buffer, place, line, base, value):
        buffer[place] = value
        return [remote(buffer.at[place], buffer.at[place], b_send.at[base + i], b_recv.at[base + i], device)
                for i, device in enumerate(line)]

    def summed(buffer, copies, count):
        for copy in copies:
            copy.wait_recv()
        value = buffer[0]
        for i in range(1, count):
            value = value + buffer[i]
        return value

    copies = share(BZ, z, along_z, 0, BV[...])
    finish(0, 1)
    give(1, 0, 1)
    give(1, 1, 2)
    copies = share(BY, y, along_y, 7, summed(BZ, copies, 8))
    give(1, 1, 3)
    give(1, 0, 2)
    copies = share(BX, x, along_x, 14, summed(BY, copies, 8))
    finish(1, 1)
    give(1, 0, 3)
    finish(0, 0)
    BM[...] = summed(BX, copies, 4) * (65536.0**-0.5)
    BT[c] = BM[...]
    last = remote(BM, BT.at[c], b_send.at[17], b_recv.at[17], partner)
    finish(1, 0)
    for gi in range(2):
        ks[gi].wait_recv()
        gk[:, cols((2 * other + gi) * 128, 128)] = KR[gi, :, 0:128]
        gv[:, cols((2 * other + gi) * 128, 128)] = KR[gi, :, 128:256]
    last.wait_recv()
    for i in range(2):
        bias[i * 16:i * 16 + 16, :] = BT[i, 0:16, :]
        bias[32 + 2 * i:34 + 2 * i, :] = BT[i, 16:18, :]
    for copy in core[6:]:
        copy.wait_recv()
    for copy in outs:
        copy.wait()
    for copy in sent:
        copy.wait_send()


def stepped(q, k, v, g, plan, first):
    dma = pltpu.SemaphoreType.DMA
    return pl.pallas_call(
        step_kernel,
        out_shape=(
            jax.ShapeDtypeStruct((128, 4096), BF16),
            jax.ShapeDtypeStruct((128, 4096), BF16),
            jax.ShapeDtypeStruct((128, 512), BF16),
            jax.ShapeDtypeStruct((128, 512), BF16),
            jax.ShapeDtypeStruct((36, 128), F32),
        ),
        in_specs=[HBM] * 4 + [VMEM] * 2,
        out_specs=(ANY, ANY, VMEM, VMEM, VMEM),
        scratch_shapes=[
            pltpu.VMEM((2, 2, 8, 256, 256), BF16),
            pltpu.VMEM((256, 2048), BF16),
            pltpu.VMEM((256, 2048), BF16),
            pltpu.VMEM((32, 1, 128), jnp.int32),
            pltpu.VMEM((32, 128), jnp.int32),
            pltpu.VMEM((32, 256), jnp.int32),
            pltpu.VMEM((32, 128), jnp.int32),
            pltpu.VMEM((2, 24, 128), F32),
            pltpu.VMEM((544, 2048), BF16),
            pltpu.VMEM((544, 2048), BF16),
            pltpu.VMEM((512, 2048), BF16),
            pltpu.VMEM((512, 2048), BF16),
            pltpu.VMEM((2, 33, 256, 256), BF16),
            pltpu.VMEM((2, 2, 8, 256, 256), BF16),
            pltpu.VMEM((256, 2048), BF16),
            pltpu.VMEM((256, 2048), BF16),
            pltpu.VMEM((24, 128), F32),
            pltpu.VMEM((4, 2, 4, 256, 256), BF16),
            pltpu.VMEM((2, 256, 256), BF16),
            pltpu.VMEM((2, 256, 256), BF16),
            pltpu.VMEM((2, 128, 256), BF16),
            pltpu.VMEM((2, 128, 256), BF16),
            pltpu.VMEM((8, 24, 128), F32),
            pltpu.VMEM((8, 24, 128), F32),
            pltpu.VMEM((4, 24, 128), F32),
            pltpu.VMEM((24, 128), F32),
            dma((6,)), dma((6,)), dma((6,)), dma((2,)), dma((2,)), dma((4, 2, 4)), dma((4, 2, 4)), dma((9,)), dma((9,)),
            dma((2,)), dma((2,)), dma((2,)), dma((2,)), dma((2,)), dma((2,)), dma((2,)), dma((4, 2, 4)), dma((4, 2, 4)),
            dma((18,)), dma((18,)),
        ],
        compiler_params=pltpu.CompilerParams(collective_id=0, has_side_effects=True, vmem_limit_bytes=LIMIT * 2**20),
        name="step",
    )(q, k, v, g, plan, first)


def place_kernel(*refs):
    kept, (arrive, leave) = refs[10:15], refs[15:]
    for way, sem in ((0, arrive), (1, leave)):
        copies = []
        for i in range(5):
            pair = (refs[i], kept[i]) if way == 0 else (kept[i], refs[i + 5])
            copies.append(pltpu.make_async_copy(pair[0], pair[1], sem.at[i]))
        if way == 0:
            for copy in copies:
                copy.start()
            first = copies
        else:
            for i in range(5):
                first[i].wait()
                copies[i].start()
            for copy in copies:
                copy.wait()


def placed(*values):
    return pl.pallas_call(
        place_kernel,
        out_shape=tuple(jax.ShapeDtypeStruct(value.shape, value.dtype) for value in values),
        in_specs=[HBM] * 5,
        out_specs=(HBM,) * 5,
        scratch_shapes=[pltpu.VMEM(value.shape, value.dtype) for value in values] + [pltpu.SemaphoreType.DMA((5,))] * 2,
        compiler_params=pltpu.CompilerParams(vmem_limit_bytes=LIMIT * 2**20),
        name="place",
    )(*values)


def local(query_rows, key_rows, value_rows, out_grad, destination, group_first):
    outs = stepped(query_rows, key_rows, value_rows, out_grad, destination.reshape(32, 128), group_first)
    att, gq, gk, gv, bias = placed(*outs)
    return att, gq, gk, gv, bias.reshape(4608)


def solution(mesh):
    rows = P(("dp", "ctx"), None)
    return jax.shard_map(
        local, mesh=mesh, in_specs=(rows, rows, rows, rows, P("dp", None), P("dp", "ctx")),
        out_specs=(rows, rows, rows, rows, P()), check_vma=False)
```

```python
import jax
import jax.numpy as jnp
from jax import lax
from jax.experimental import pallas as pl
from jax.experimental.pallas import tpu as pltpu
from jax.sharding import PartitionSpec as P

MESH = pl.DeviceIdType.MESH
VMEM = pl.BlockSpec(memory_space=pltpu.VMEM)
ANY = pl.BlockSpec(memory_space=pl.ANY)
HBM = pl.BlockSpec(memory_space=pltpu.HBM)
LIMIT = 62
F32 = jnp.float32
BF16 = jnp.bfloat16


def places():
    dp = lax.axis_index("dp")
    ctx = lax.axis_index("ctx")
    return dp, ctx, ctx // 16, lax.rem(ctx // 2, 8), lax.rem(ctx, 2)


def at_ctx(dp, yh, z, c):
    return (dp, yh * 16 + z * 2 + c)


def cols(start, size):
    return pl.ds(pl.multiple_of(start, 128), size)


SCALE = 128**-0.5
LOG2E = 1.4426950408889634
GROUPS = 4


def dot(a, b, ca, cb):
    return lax.dot_general(a, b, (((ca,), (cb,)), ((), ())), preferred_element_type=F32)


def step_kernel(q, k, v, g, plan, first, att, gq, gk, gv, bias,
                KV, QX, GX, LK, PS, PP, PQ, BT, QP, GP, OP, DQP, PAD, D, ATT, GQ, BV, R, YS, YR, KS, KR, BZ, BY, BX, BM, YX,
                local_sem, core_send, core_recv, y_send, y_recv, z_send, z_recv, l_send, l_recv,
                out_sem, o_send, o_recv, k_send, k_recv, v_send, v_recv, r_send, r_recv, b_send, b_recv, j_send, j_recv, x_send, x_recv):
    dp, ctx, yh, z, c = places()
    yl, x = dp // 4, lax.rem(dp, 4)
    y = yh * 4 + yl
    other = 1 - c
    half = pl.ds(0, 128), pl.ds(128, 128)
    mine = pl.ds(pl.multiple_of(c * 128, 128), 128)
    theirs = pl.ds(pl.multiple_of(other * 128, 128), 128)
    chip = yh * 8 + z

    def copied(src, dst, sem):
        copy = pltpu.make_async_copy(src, dst, sem)
        copy.start()
        return copy

    local = []
    for gi in range(2):
        at = cols((2 * c + gi) * 128, 128)
        local.append(copied(k.at[:, at], KV.at[gi, yh, z, mine, half[0]], local_sem.at[2 * gi]))
        local.append(copied(v.at[:, at], KV.at[gi, yh, z, mine, half[1]], local_sem.at[2 * gi + 1]))
    local.append(copied(q.at[:, cols(c * 2048, 2048)], QX.at[mine, :], local_sem.at[4]))
    local.append(copied(g.at[:, cols(c * 2048, 2048)], GX.at[mine, :], local_sem.at[5]))
    flag = c * 16 + yh * 8 + z
    LK[flag] = (jnp.broadcast_to(first[...], (1, 128)) < ctx).astype(jnp.int32)

    def at_y(yy):
        return (lax.rem(yy, 4) * 4 + x, (yy // 4) * 16 + z * 2 + c)

    partner = at_ctx(dp, yh, z, other)
    across = at_ctx(dp, 1 - yh, z, c)
    along_z = [at_ctx(dp, yh, lax.rem(z + i, 8), c) for i in range(1, 8)]
    along_y = [at_y(lax.rem(y + i, 8)) for i in range(1, 8)]
    along_x = [(yl * 4 + lax.rem(x + i, 4), ctx) for i in range(1, 4)]
    right, left = along_z[0], along_z[6]
    barrier = pltpu.get_barrier_semaphore()
    for device in along_z + along_y + along_x + [partner]:
        pl.semaphore_signal(barrier, inc=1, device_id=device, device_id_type=MESH)
    pl.semaphore_wait(barrier, 18)

    sent = []

    def remote(src, dst, send, recv, device):
        copy = pltpu.make_async_remote_copy(src_ref=src, dst_ref=dst, send_sem=send, recv_sem=recv,
                                            device_id=device, device_id_type=MESH)
        copy.start()
        sent.append(copy)
        return copy

    core = []
    for gi in range(2):
        at = cols((2 * other + gi) * 128, 128)
        for j, src in ((0, k), (1, v)):
            i = 2 * gi + j
            core.append(remote(src.at[:, at], KV.at[gi, yh, z, mine, half[j]], core_send.at[i], core_recv.at[i], partner))
    for i, (src, dst) in ((4, (q, QX)), (5, (g, GX))):
        core.append(remote(src.at[:, cols(other * 2048, 2048)], dst.at[mine, :], core_send.at[i], core_recv.at[i],
                           partner))

    def side(far):
        return 1 - yh if far else yh

    def ring(zz):
        return lax.rem(zz + 8, 8)

    def placing(c):
        at = lax.broadcasted_iota(jnp.int32, (512, 128), 0)
        return jnp.concatenate([(PS[pl.ds(2 * c + i, 1), :] == at).astype(BF16) for i in range(2)], axis=1)

    def tables():
        def iota(shape, dim):
            return lax.broadcasted_iota(jnp.int32, shape, dim)

        block = plan[...] // 128
        spot = plan[...] - block * 128
        found = jnp.concatenate([block, spot + 1], axis=0).astype(F32)
        found = jnp.concatenate([found, jnp.zeros((64, 128), F32)], axis=0).T.astype(BF16)
        lane = iota((128, 1024), 1)
        device = (iota((128, 1024), 0) == lane // 32).astype(BF16)
        inside = dot(found, device, 1, 0) == (lane % 32).astype(F32)
        member = inside.astype(BF16)
        earlier = dot((iota((128, 128), 0) > iota((128, 128), 1)).astype(BF16), member, 1, 0)
        ranks = dot(jnp.where(inside, earlier, 0.0).astype(BF16), device, 1, 1)
        PS[...] = block * 16 + iota((32, 128), 0) % 2 * 8 + ranks.T[0:32].astype(jnp.int32)
        lane = iota((128, 256), 1)
        row = iota((128, 256), 0)
        rank = dot(ranks.astype(BF16), (row == lane // 8).astype(BF16), 1, 0)
        value = dot(found, (row == lane // 8 + 32).astype(BF16), 1, 0)
        filled = jnp.where(rank == (lane % 8).astype(F32), value, 0.0).astype(BF16)
        every = dot(member, filled, 0, 0)
        lane = iota((32, 256), 1) // 8
        table = jnp.zeros((32, 256), F32)
        for i in range(32):
            table = table + jnp.where(lane == i, every[i * 32:i * 32 + 32], 0.0)
        PP[...] = table.astype(jnp.int32)
        own = (iota((256, 128), 0) == chip * 16 + iota((256, 128), 1) % 16).astype(BF16)
        own = dot(table.astype(BF16), own, 1, 0).astype(jnp.int32)
        PQ[...] = jnp.where(own == 0, 127, own - 1)

    def widen(gi, far, zs):
        found = [dot(placing(side(far) * 8 + zz), KV[gi, side(far), zz], 1, 0).astype(BF16) for zz in zs]
        for zz, rows in zip(zs, found):
            at = pl.ds(pl.multiple_of((side(far) * 8 + zz) * 16, 16), 16)
            PAD[gi, 1:33, at, :] = rows.reshape(32, 16, 256)

    rows = {}
    ys = {}
    jumps = {}

    def bring(gi, far, s, later=False):
        item = 2 * far + gi
        if s == 0 and far:
            ys[gi].wait_recv()
        elif s == 0:
            for i in (2 * gi, 2 * gi + 1):
                core[i].wait_recv()
        if far and s == 4:
            jumps[gi].wait_recv()
        for way in range(2):
            if 0 < s < 5 - far:
                rows[(item, way, s - 1)].wait_recv()
                if s == 1 and not far:
                    rows[(item, way, 4)].wait_recv()
            if s < 4 - far:
                ref = KV.at[gi, side(far), ring(z - s if way == 0 else z + s)]
                if s == 3:
                    ref = ref.at[half[way], :]
                elif s == 0 and not far:
                    ref = ref.at[theirs, :]
                rows[(item, way, s)] = remote(ref, ref, z_send.at[item, way, s], z_recv.at[item, way, s],
                                              right if way == 0 else left)
        if s == 0 and not far:
            ref = KV.at[gi, yh, z]
            ys[gi] = remote(ref, ref, y_send.at[gi], y_recv.at[gi], across)
        if s == 4 and not far:
            ref = KV.at[gi, yh, ring(z + 4)]
            jumps[gi] = remote(ref, ref, j_send.at[gi], j_recv.at[gi], across)
        if not later:
            widen(gi, far, [ring(z + s)] if s in (0, 4) else [ring(z - s), ring(z + s)])

    def lead(gi):
        for i in (2 * gi, 2 * gi + 1):
            local[i].wait()
        ref = KV.at[gi, yh, z, mine, :]
        for way in range(2):
            rows[(gi, way, 4)] = remote(ref, ref, z_send.at[gi, way, 4], z_recv.at[gi, way, 4],
                                        right if way == 0 else left)

    def queries(ref, gi, b):
        at = slice(b * 16 + 16, b * 16 + 32)
        return jnp.concatenate([ref[at, (gi * 8 + h) * 128:(gi * 8 + h + 1) * 128] for h in range(8)], axis=0)

    def seat(b):
        return (PP[b:b + 1, :] == lax.broadcasted_iota(jnp.int32, (128, 256), 0) + 1).astype(BF16)

    def unseat(gi, dk, dv, b):
        grads = [jnp.concatenate([dk[j], dv[j]], axis=1).astype(BF16) for j in range(len(b))]
        back = [dot(seat(b[j]), grads[j], 0, 0).astype(BF16) for j in range(len(b))]
        for j in range(len(b)):
            PAD[gi, b[j] + 1] = back[j]

    def blocks(gi, i, carry):
        s_last, p_last, w_last, sl_last, kv_last, total = carry
        un = 32 // GROUPS
        span = range(un)
        b = [i * un + j for j in span]
        kv = [dot(seat(b[j]), PAD[gi, b[j] + 1], 1, 0).astype(BF16) for j in span]
        qs = [queries(QP, gi, b[0] + j - 1) for j in range(un + 2)]
        os = [queries(GP, gi, b[0] + j - 1) for j in range(un + 2)]
        s = [dot(kv[j][:, 0:128], jnp.concatenate([qs[j + 1], qs[j + 2]], axis=0), 1, 1) for j in span]
        p = [dot(kv[j][:, 128:256], jnp.concatenate([os[j + 1], os[j + 2]], axis=0), 1, 1) for j in span]
        u = lax.broadcasted_iota(jnp.int32, (128, 128), 0)
        s_own = [jnp.where(u <= PQ[b[j]:b[j] + 1, :], s[j][:, 0:128], -jnp.inf) for j in span]
        s_pri = [jnp.where(jnp.broadcast_to(LK[seen_at(b[j])] > 0, (128, 128)), s[j - 1][:, 128:256] if j else s_last, -jnp.inf)
                 for j in span]
        p_own = [p[j][:, 0:128] for j in span]
        p_pri = [p[j - 1][:, 128:256] if j else p_last for j in span]
        top = [jnp.max(jnp.maximum(s_own[j], s_pri[j]), axis=0, keepdims=True) for j in span]
        e_own = [jnp.exp2((s_own[j] - top[j]) * (SCALE * LOG2E)) for j in span]
        e_pri = [jnp.exp2((s_pri[j] - top[j]) * (SCALE * LOG2E)) for j in span]
        inv = [1.0 / jnp.sum(e_own[j] + e_pri[j], axis=0, keepdims=True) for j in span]
        w_own = [e_own[j] * inv[j] for j in span]
        w_pri = [e_pri[j] * inv[j] for j in span]
        centred = [jnp.sum(w_own[j] * p_own[j] + w_pri[j] * p_pri[j], axis=0, keepdims=True) for j in span]
        sl_own = [((w_own[j] * (p_own[j] - centred[j])) * SCALE).astype(BF16) for j in span]
        sl_pri = [((w_pri[j] * (p_pri[j] - centred[j])) * SCALE).astype(BF16) for j in span]
        w_own = [w.astype(BF16) for w in w_own]
        w_pri = [w.astype(BF16) for w in w_pri]
        att, gq, dk, dv = [], [], [], []
        for j in span:
            pair = jnp.concatenate([kv[j - 1] if j else kv_last, kv[j]], axis=0)
            att.append(dot(jnp.concatenate([w_pri[j], w_own[j]], axis=0), pair[:, 128:256], 0, 0).astype(BF16))
            gq.append(dot(jnp.concatenate([sl_pri[j], sl_own[j]], axis=0), pair[:, 0:128], 0, 0).astype(BF16))
            dk.append(dot(jnp.concatenate([sl_own[j - 1] if j else sl_last, sl_pri[j]], axis=1),
                          jnp.concatenate([qs[j], qs[j + 1]], axis=0), 1, 0))
            dv.append(dot(jnp.concatenate([w_own[j - 1] if j else w_last, w_pri[j]], axis=1),
                          jnp.concatenate([os[j], os[j + 1]], axis=0), 1, 0))
        for j in span:
            at = slice(b[j] * 16, b[j] * 16 + 16)
            for h in range(8):
                to = slice((gi * 8 + h) * 128, (gi * 8 + h + 1) * 128)
                OP[at, to] = att[j][h * 16:(h + 1) * 16]
                DQP[at, to] = gq[j][h * 16:(h + 1) * 16]
        first = 0 if i else 1
        unseat(gi, dk[first:], dv[first:], [bj - 1 for bj in b[first:]])
        for j in span[first:]:
            total = total + jnp.sum(dv[j].reshape(16, 8, 128), axis=0)
        if i == GROUPS - 1:
            dk = dot(sl_own[-1], qs[un], 1, 0)
            dv = dot(w_own[-1], os[un], 1, 0)
            unseat(gi, [dk], [dv], [31])
            total = total + jnp.sum(dv.reshape(16, 8, 128), axis=0)
            BV[16 + gi:17 + gi, :] = jnp.sum(total, axis=0, keepdims=True)
        return s[-1][:, 128:256], p[-1][:, 128:256], w_own[-1], sl_own[-1], kv[-1], total

    def seen_at(b):
        return b % 2 * 16 + b // 16 * 8 + b // 2 % 8

    def opening():
        zf = jnp.zeros((128, 128), F32)
        zb = jnp.zeros((128, 128), BF16)
        return zf, zf, zb, zb, jnp.zeros((128, 256), BF16), jnp.zeros((8, 128), F32)

    def narrow(gi, places):
        out = []
        for far, zz in places:
            at = pl.ds(pl.multiple_of((side(far) * 8 + zz) * 16, 16), 16)
            wide = PAD[gi, 1:33, at, :].reshape(512, 256)
            out.append(dot(placing(side(far) * 8 + zz), wide, 0, 0).astype(BF16))
        for (far, zz), value in zip(places, out):
            D[gi, side(far), zz] = value

    back = {}

    def give(gi, far, s):
        item = 2 * far + gi
        for way in range(2):
            target = z + 4 - s if way == 0 else z - 4 + s
            term = D.at[gi, side(far), ring(target)]
            dst = R.at[item, way, s]
            if s == 0:
                if way == 0:
                    jumps[gi].wait_recv()
                    YX[gi] = (YX[gi].astype(F32) + term[...].astype(F32)).astype(BF16)
                src = YX.at[gi, half[way], :]
                dst = dst.at[half[way], :]
            elif far and s == 1:
                src = term
            else:
                back[(item, way, s - 1)].wait_recv()
                src = R.at[item, way, s - 1]
                for part in range(2):
                    at = slice(part * 128, part * 128 + 128)
                    if s == 1 and part != way:
                        src[at, :] = term[at, :]
                    else:
                        src[at, :] = (src[at, :].astype(F32) + term[at, :].astype(F32)).astype(BF16)
            back[(item, way, s)] = remote(src, dst, r_send.at[item, way, s], r_recv.at[item, way, s],
                                          right if way == 0 else left)

    def total(gi, far, at):
        item = 2 * far + gi
        return (D[gi, side(far), z, at, :].astype(F32) + R[item, 0, 3, at, :].astype(F32)
                + R[item, 1, 3, at, :].astype(F32))

    def finish(gi, far):
        item = 2 * far + gi
        back[(item, 0, 3)].wait_recv()
        back[(item, 1, 3)].wait_recv()
        if far:
            YS[gi] = total(gi, 1, slice(0, 256)).astype(BF16)
            ys[gi] = remote(YS.at[gi], YR.at[gi], v_send.at[gi], v_recv.at[gi], across)
            return
        ys[gi].wait_recv()
        KS[gi] = (total(gi, 0, theirs) + YR[gi, theirs, :].astype(F32)).astype(BF16)
        ks.append(remote(KS.at[gi], KR.at[gi], k_send.at[gi], k_recv.at[gi], partner))
        done = (total(gi, 0, mine) + YR[gi, mine, :].astype(F32)).astype(BF16)
        gk[:, cols((2 * c + gi) * 128, 128)] = done[:, 0:128]
        gv[:, cols((2 * c + gi) * 128, 128)] = done[:, 128:256]

    def start_reduce(gi):
        narrow(gi, [(1, ring(z + 4)), (1, ring(z + 3)), (1, ring(z + 5))])
        jumps[gi] = remote(D.at[gi, side(1), ring(z + 4)], YX.at[gi], x_send.at[gi], x_recv.at[gi], across)
        give(gi, 1, 1)
        narrow(gi, [(far, ring(z + i)) for i in (2, 6) for far in (1, 0)])
        narrow(gi, [(1, ring(z + 1)), (1, ring(z + 7)), (0, ring(z + 4)), (0, ring(z + 3)), (0, ring(z + 5))])
        narrow(gi, [(0, ring(z + 1)), (0, ring(z + 7)), (1, z), (0, z)])

    ks = []

    lead(0)
    lead(1)
    bring(0, 0, 0, later=True)
    bring(1, 0, 0, later=True)
    flags = [remote(LK.at[flag], LK.at[flag], l_send.at[i], l_recv.at[i], along_z[i]) for i in range(7)]
    tables()
    BV[...] = jnp.zeros_like(BV)
    zeros = jnp.zeros((16, 2048), BF16)
    for ref in (QP, GP):
        ref[0:16, :] = zeros
        ref[528:544, :] = zeros
    for gi in range(2):
        widen(gi, 0, [z])
    for i in (4, 5):
        local[i].wait()
        core[i].wait_recv()
    here = placing(chip)

    def spread(ref, src, j):
        at = slice(j * 256, (j + 1) * 256)
        ref[16:528, at] = dot(here, src[:, at], 1, 0).astype(BF16)

    for j in range(4):
        spread(QP, QX, j)
    bring(0, 0, 1)
    for copy in flags:
        copy.wait_recv()
    part = pl.ds(c * 16 + yh * 8, 8)
    flag_y = remote(LK.at[part], LK.at[part], l_send.at[7], l_recv.at[7], across)
    for j in range(4):
        spread(GP, GX, j)
    bring(1, 0, 1)
    for j in range(4, 8):
        spread(QP, QX, j)
    bring(0, 0, 2)
    bring(0, 1, 0)
    flag_y.wait_recv()
    part = pl.ds(c * 16, 16)
    flag_core = remote(LK.at[part], LK.at[part], l_send.at[8], l_recv.at[8], partner)
    for j in range(4, 8):
        spread(GP, GX, j)
    bring(0, 0, 3)
    bring(0, 1, 1)
    bring(0, 0, 4)
    bring(1, 0, 2)
    bring(0, 1, 2)
    flag_core.wait_recv()
    bring(1, 0, 3)
    bring(0, 1, 3)
    bring(1, 1, 0)
    bring(0, 1, 4)
    bring(1, 0, 4)
    carry = blocks(0, 0, opening())
    bring(1, 1, 1)
    carry = blocks(0, 1, carry)
    carry = blocks(0, 2, carry)
    bring(1, 1, 2)
    carry = blocks(0, 3, carry)
    start_reduce(0)
    bring(1, 1, 3)
    bring(1, 1, 4)
    carry = blocks(1, 0, opening())
    give(0, 1, 2)
    carry = blocks(1, 1, carry)
    carry = blocks(1, 2, carry)
    give(0, 1, 3)
    give(0, 0, 0)
    carry = blocks(1, 3, carry)
    start_reduce(1)
    give(0, 0, 1)
    here = placing(chip)
    for j in range(8):
        at = slice(j * 256, (j + 1) * 256)
        ATT[:, at] = dot(here, OP[:, at], 0, 0).astype(BF16)
        wide = dot(here, DQP[:, at], 0, 0)
        GQ[:, at] = wide.astype(BF16)
        sums = jnp.sum(wide, axis=0, keepdims=True)
        BV[2 * j:2 * j + 1, :] = sums[:, 0:128]
        BV[2 * j + 1:2 * j + 2, :] = sums[:, 128:256]
    outs = []
    for i, (src, dst) in enumerate(((ATT, att), (GQ, gq))):
        outs.append(copied(src.at[mine, :], dst.at[:, cols(c * 2048, 2048)], out_sem.at[i]))
        core.append(remote(src.at[theirs, :], dst.at[:, cols(c * 2048, 2048)], o_send.at[i], o_recv.at[i], partner))

    def share(buffer, place, line, base, value):
        buffer[place] = value
        return [remote(buffer.at[place], buffer.at[place], b_send.at[base + i], b_recv.at[base + i], device)
                for i, device in enumerate(line)]

    def summed(buffer, copies, count):
        for copy in copies:
            copy.wait_recv()
        value = buffer[0]
        for i in range(1, count):
            value = value + buffer[i]
        return value

    copies = share(BZ, z, along_z, 0, BV[...])
    give(1, 1, 2)
    finish(0, 1)
    give(0, 0, 2)
    copies = share(BY, y, along_y, 7, summed(BZ, copies, 8))
    give(1, 0, 0)
    give(1, 1, 3)
    give(1, 0, 1)
    give(0, 0, 3)
    finish(1, 1)
    give(1, 0, 2)
    copies = share(BX, x, along_x, 14, summed(BY, copies, 8))
    finish(0, 0)
    give(1, 0, 3)
    finish(1, 0)
    BM[...] = summed(BX, copies, 4) * (65536.0**-0.5)
    BT[c] = BM[...]
    last = remote(BM, BT.at[c], b_send.at[17], b_recv.at[17], partner)
    for gi in range(2):
        ks[gi].wait_recv()
        gk[:, cols((2 * other + gi) * 128, 128)] = KR[gi, :, 0:128]
        gv[:, cols((2 * other + gi) * 128, 128)] = KR[gi, :, 128:256]
    last.wait_recv()
    for i in range(2):
        bias[i * 16:i * 16 + 16, :] = BT[i, 0:16, :]
        bias[32 + 2 * i:34 + 2 * i, :] = BT[i, 16:18, :]
    for copy in core[6:]:
        copy.wait_recv()
    for copy in outs:
        copy.wait()
    for copy in sent:
        copy.wait_send()


def stepped(q, k, v, g, plan, first):
    dma = pltpu.SemaphoreType.DMA
    return pl.pallas_call(
        step_kernel,
        out_shape=(
            jax.ShapeDtypeStruct((128, 4096), BF16),
            jax.ShapeDtypeStruct((128, 4096), BF16),
            jax.ShapeDtypeStruct((128, 512), BF16),
            jax.ShapeDtypeStruct((128, 512), BF16),
            jax.ShapeDtypeStruct((36, 128), F32),
        ),
        in_specs=[HBM] * 4 + [VMEM] * 2,
        out_specs=(ANY, ANY, VMEM, VMEM, VMEM),
        scratch_shapes=[
            pltpu.VMEM((2, 2, 8, 256, 256), BF16),
            pltpu.VMEM((256, 2048), BF16),
            pltpu.VMEM((256, 2048), BF16),
            pltpu.VMEM((32, 1, 128), jnp.int32),
            pltpu.VMEM((32, 128), jnp.int32),
            pltpu.VMEM((32, 256), jnp.int32),
            pltpu.VMEM((32, 128), jnp.int32),
            pltpu.VMEM((2, 24, 128), F32),
            pltpu.VMEM((544, 2048), BF16),
            pltpu.VMEM((544, 2048), BF16),
            pltpu.VMEM((512, 2048), BF16),
            pltpu.VMEM((512, 2048), BF16),
            pltpu.VMEM((2, 33, 256, 256), BF16),
            pltpu.VMEM((2, 2, 8, 256, 256), BF16),
            pltpu.VMEM((256, 2048), BF16),
            pltpu.VMEM((256, 2048), BF16),
            pltpu.VMEM((24, 128), F32),
            pltpu.VMEM((4, 2, 4, 256, 256), BF16),
            pltpu.VMEM((2, 256, 256), BF16),
            pltpu.VMEM((2, 256, 256), BF16),
            pltpu.VMEM((2, 128, 256), BF16),
            pltpu.VMEM((2, 128, 256), BF16),
            pltpu.VMEM((8, 24, 128), F32),
            pltpu.VMEM((8, 24, 128), F32),
            pltpu.VMEM((4, 24, 128), F32),
            pltpu.VMEM((24, 128), F32),
            pltpu.VMEM((2, 256, 256), BF16),
            dma((6,)), dma((6,)), dma((6,)), dma((2,)), dma((2,)), dma((4, 2, 5)), dma((4, 2, 5)), dma((9,)), dma((9,)),
            dma((2,)), dma((2,)), dma((2,)), dma((2,)), dma((2,)), dma((2,)), dma((2,)), dma((4, 2, 4)), dma((4, 2, 4)),
            dma((18,)), dma((18,)), dma((2,)), dma((2,)), dma((2,)), dma((2,)),
        ],
        compiler_params=pltpu.CompilerParams(collective_id=0, has_side_effects=True, vmem_limit_bytes=LIMIT * 2**20),
        name="step",
    )(q, k, v, g, plan, first)


def place_kernel(*refs):
    kept, (arrive, leave) = refs[10:15], refs[15:]
    for way, sem in ((0, arrive), (1, leave)):
        copies = []
        for i in range(5):
            pair = (refs[i], kept[i]) if way == 0 else (kept[i], refs[i + 5])
            copies.append(pltpu.make_async_copy(pair[0], pair[1], sem.at[i]))
        if way == 0:
            for copy in copies:
                copy.start()
            first = copies
        else:
            for i in range(5):
                first[i].wait()
                copies[i].start()
            for copy in copies:
                copy.wait()


def placed(*values):
    return pl.pallas_call(
        place_kernel,
        out_shape=tuple(jax.ShapeDtypeStruct(value.shape, value.dtype) for value in values),
        in_specs=[HBM] * 5,
        out_specs=(HBM,) * 5,
        scratch_shapes=[pltpu.VMEM(value.shape, value.dtype) for value in values] + [pltpu.SemaphoreType.DMA((5,))] * 2,
        compiler_params=pltpu.CompilerParams(vmem_limit_bytes=LIMIT * 2**20),
        name="place",
    )(*values)


def local(query_rows, key_rows, value_rows, out_grad, destination, group_first):
    outs = stepped(query_rows, key_rows, value_rows, out_grad, destination.reshape(32, 128), group_first)
    att, gq, gk, gv, bias = placed(*outs)
    return att, gq, gk, gv, bias.reshape(4608)


def solution(mesh):
    rows = P(("dp", "ctx"), None)
    return jax.shard_map(
        local, mesh=mesh, in_specs=(rows, rows, rows, rows, P("dp", None), P("dp", "ctx")),
        out_specs=(rows, rows, rows, rows, P()), check_vma=False)
```

```python
import jax
import jax.numpy as jnp
from jax import lax
from jax.experimental import pallas as pl
from jax.experimental.pallas import tpu as pltpu
from jax.sharding import PartitionSpec as P

MESH = pl.DeviceIdType.MESH
VMEM = pl.BlockSpec(memory_space=pltpu.VMEM)
ANY = pl.BlockSpec(memory_space=pl.ANY)
HBM = pl.BlockSpec(memory_space=pltpu.HBM)
LIMIT = 62
F32 = jnp.float32
BF16 = jnp.bfloat16


def places():
    dp = lax.axis_index("dp")
    ctx = lax.axis_index("ctx")
    return dp, ctx, ctx // 16, lax.rem(ctx // 2, 8), lax.rem(ctx, 2)


def at_ctx(dp, yh, z, c):
    return (dp, yh * 16 + z * 2 + c)


def cols(start, size):
    return pl.ds(pl.multiple_of(start, 128), size)


SCALE = 128**-0.5
LOG2E = 1.4426950408889634
GROUPS = 4


def dot(a, b, ca, cb):
    return lax.dot_general(a, b, (((ca,), (cb,)), ((), ())), preferred_element_type=F32)


def step_kernel(q, k, v, g, plan, first, att, gq, gk, gv, bias,
                KV, QX, GX, LK, PS, PP, PQ, BT, QP, GP, OP, DQP, PAD, D, ATT, GQ, BV, R, YS, YR, KS, KR, BZ, BY, BX, BM, YX,
                local_sem, core_send, core_recv, y_send, y_recv, z_send, z_recv, l_send, l_recv,
                out_sem, o_send, o_recv, k_send, k_recv, v_send, v_recv, r_send, r_recv, b_send, b_recv, j_send, j_recv, x_send, x_recv):
    dp, ctx, yh, z, c = places()
    yl, x = dp // 4, lax.rem(dp, 4)
    y = yh * 4 + yl
    other = 1 - c
    half = pl.ds(0, 128), pl.ds(128, 128)
    mine = pl.ds(pl.multiple_of(c * 128, 128), 128)
    theirs = pl.ds(pl.multiple_of(other * 128, 128), 128)
    chip = yh * 8 + z

    def copied(src, dst, sem):
        copy = pltpu.make_async_copy(src, dst, sem)
        copy.start()
        return copy

    local = []
    for gi in range(2):
        at = cols((2 * c + gi) * 128, 128)
        local.append(copied(k.at[:, at], KV.at[gi, yh, z, mine, half[0]], local_sem.at[2 * gi]))
        local.append(copied(v.at[:, at], KV.at[gi, yh, z, mine, half[1]], local_sem.at[2 * gi + 1]))
    local.append(copied(q.at[:, cols(c * 2048, 2048)], QX.at[mine, :], local_sem.at[4]))
    local.append(copied(g.at[:, cols(c * 2048, 2048)], GX.at[mine, :], local_sem.at[5]))
    flag = c * 16 + yh * 8 + z
    LK[flag] = (jnp.broadcast_to(first[...], (1, 128)) < ctx).astype(jnp.int32)

    def at_y(yy):
        return (lax.rem(yy, 4) * 4 + x, (yy // 4) * 16 + z * 2 + c)

    partner = at_ctx(dp, yh, z, other)
    across = at_ctx(dp, 1 - yh, z, c)
    along_z = [at_ctx(dp, yh, lax.rem(z + i, 8), c) for i in range(1, 8)]
    along_y = [at_y(lax.rem(y + i, 8)) for i in range(1, 8)]
    along_x = [(yl * 4 + lax.rem(x + i, 4), ctx) for i in range(1, 4)]
    right, left = along_z[0], along_z[6]
    barrier = pltpu.get_barrier_semaphore()
    for device in along_z + along_y + along_x + [partner]:
        pl.semaphore_signal(barrier, inc=1, device_id=device, device_id_type=MESH)
    pl.semaphore_wait(barrier, 18)

    sent = []

    def remote(src, dst, send, recv, device):
        copy = pltpu.make_async_remote_copy(src_ref=src, dst_ref=dst, send_sem=send, recv_sem=recv,
                                            device_id=device, device_id_type=MESH)
        copy.start()
        sent.append(copy)
        return copy

    core = []
    for gi in range(2):
        at = cols((2 * other + gi) * 128, 128)
        for j, src in ((0, k), (1, v)):
            i = 2 * gi + j
            core.append(remote(src.at[:, at], KV.at[gi, yh, z, mine, half[j]], core_send.at[i], core_recv.at[i], partner))
    for i, (src, dst) in ((4, (q, QX)), (5, (g, GX))):
        core.append(remote(src.at[:, cols(other * 2048, 2048)], dst.at[mine, :], core_send.at[i], core_recv.at[i],
                           partner))

    def side(far):
        return 1 - yh if far else yh

    def ring(zz):
        return lax.rem(zz + 8, 8)

    def placing(c):
        at = lax.broadcasted_iota(jnp.int32, (512, 128), 0)
        return jnp.concatenate([(PS[pl.ds(2 * c + i, 1), :] == at).astype(BF16) for i in range(2)], axis=1)

    def tables():
        def iota(shape, dim):
            return lax.broadcasted_iota(jnp.int32, shape, dim)

        block = plan[...] // 128
        spot = plan[...] - block * 128
        found = jnp.concatenate([block, spot + 1], axis=0).astype(F32)
        found = jnp.concatenate([found, jnp.zeros((64, 128), F32)], axis=0).T.astype(BF16)
        lane = iota((128, 1024), 1)
        device = (iota((128, 1024), 0) == lane // 32).astype(BF16)
        inside = dot(found, device, 1, 0) == (lane % 32).astype(F32)
        member = inside.astype(BF16)
        earlier = dot((iota((128, 128), 0) > iota((128, 128), 1)).astype(BF16), member, 1, 0)
        ranks = dot(jnp.where(inside, earlier, 0.0).astype(BF16), device, 1, 1)
        PS[...] = block * 16 + iota((32, 128), 0) % 2 * 8 + ranks.T[0:32].astype(jnp.int32)
        lane = iota((128, 256), 1)
        row = iota((128, 256), 0)
        rank = dot(ranks.astype(BF16), (row == lane // 8).astype(BF16), 1, 0)
        value = dot(found, (row == lane // 8 + 32).astype(BF16), 1, 0)
        filled = jnp.where(rank == (lane % 8).astype(F32), value, 0.0).astype(BF16)
        every = dot(member, filled, 0, 0)
        lane = iota((32, 256), 1) // 8
        table = jnp.zeros((32, 256), F32)
        for i in range(32):
            table = table + jnp.where(lane == i, every[i * 32:i * 32 + 32], 0.0)
        PP[...] = table.astype(jnp.int32)
        own = (iota((256, 128), 0) == chip * 16 + iota((256, 128), 1) % 16).astype(BF16)
        own = dot(table.astype(BF16), own, 1, 0).astype(jnp.int32)
        PQ[...] = jnp.where(own == 0, 127, own - 1)

    def widen(gi, far, zs):
        found = [dot(placing(side(far) * 8 + zz), KV[gi, side(far), zz], 1, 0).astype(BF16) for zz in zs]
        for zz, rows in zip(zs, found):
            at = pl.ds(pl.multiple_of((side(far) * 8 + zz) * 16, 16), 16)
            PAD[gi, 1:33, at, :] = rows.reshape(32, 16, 256)

    rows = {}
    ys = {}
    jumps = {}

    def bring(gi, far, s, later=False):
        item = 2 * far + gi
        if s == 0 and far:
            ys[gi].wait_recv()
        elif s == 0:
            for i in (2 * gi, 2 * gi + 1):
                core[i].wait_recv()
        if far and s == 4:
            jumps[gi].wait_recv()
        for part in range(2):
            for way in range(2):
                if 0 < s < 5 - far and (s < 4 or part == way):
                    rows[(item, way, s - 1, part)].wait_recv()
                if s < 4 - far and (s < 3 or part == way) and (s or far or part):
                    ref = KV.at[gi, side(far), ring(z - s if way == 0 else z + s), (mine, theirs)[part], :]
                    rows[(item, way, s, part)] = remote(ref, ref, z_send.at[item, way, s, part],
                                                        z_recv.at[item, way, s, part], right if way == 0 else left)
        if s == 0 and not far:
            ref = KV.at[gi, yh, z]
            ys[gi] = remote(ref, ref, y_send.at[gi], y_recv.at[gi], across)
        if s == 4 and not far:
            ref = KV.at[gi, yh, ring(z + 4)]
            jumps[gi] = remote(ref, ref, j_send.at[gi], j_recv.at[gi], across)
        if not later:
            widen(gi, far, [ring(z + s)] if s in (0, 4) else [ring(z - s), ring(z + s)])

    def lead(gi):
        for i in (2 * gi, 2 * gi + 1):
            local[i].wait()
        ref = KV.at[gi, yh, z, mine, :]
        for way in range(2):
            rows[(gi, way, 0, 0)] = remote(ref, ref, z_send.at[gi, way, 0, 0], z_recv.at[gi, way, 0, 0],
                                           right if way == 0 else left)

    def queries(ref, gi, b):
        at = slice(b * 16 + 16, b * 16 + 32)
        return jnp.concatenate([ref[at, (gi * 8 + h) * 128:(gi * 8 + h + 1) * 128] for h in range(8)], axis=0)

    def seat(b):
        return (PP[b:b + 1, :] == lax.broadcasted_iota(jnp.int32, (128, 256), 0) + 1).astype(BF16)

    def unseat(gi, dk, dv, b):
        grads = [jnp.concatenate([dk[j], dv[j]], axis=1).astype(BF16) for j in range(len(b))]
        back = [dot(seat(b[j]), grads[j], 0, 0).astype(BF16) for j in range(len(b))]
        for j in range(len(b)):
            PAD[gi, b[j] + 1] = back[j]

    def blocks(gi, i, carry):
        s_last, p_last, w_last, sl_last, kv_last, total = carry
        un = 32 // GROUPS
        span = range(un)
        b = [i * un + j for j in span]
        kv = [dot(seat(b[j]), PAD[gi, b[j] + 1], 1, 0).astype(BF16) for j in span]
        qs = [queries(QP, gi, b[0] + j - 1) for j in range(un + 2)]
        os = [queries(GP, gi, b[0] + j - 1) for j in range(un + 2)]
        s = [dot(kv[j][:, 0:128], jnp.concatenate([qs[j + 1], qs[j + 2]], axis=0), 1, 1) for j in span]
        p = [dot(kv[j][:, 128:256], jnp.concatenate([os[j + 1], os[j + 2]], axis=0), 1, 1) for j in span]
        u = lax.broadcasted_iota(jnp.int32, (128, 128), 0)
        s_own = [jnp.where(u <= PQ[b[j]:b[j] + 1, :], s[j][:, 0:128], -jnp.inf) for j in span]
        s_pri = [jnp.where(jnp.broadcast_to(LK[seen_at(b[j])] > 0, (128, 128)), s[j - 1][:, 128:256] if j else s_last, -jnp.inf)
                 for j in span]
        p_own = [p[j][:, 0:128] for j in span]
        p_pri = [p[j - 1][:, 128:256] if j else p_last for j in span]
        top = [jnp.max(jnp.maximum(s_own[j], s_pri[j]), axis=0, keepdims=True) for j in span]
        e_own = [jnp.exp2((s_own[j] - top[j]) * (SCALE * LOG2E)) for j in span]
        e_pri = [jnp.exp2((s_pri[j] - top[j]) * (SCALE * LOG2E)) for j in span]
        inv = [1.0 / jnp.sum(e_own[j] + e_pri[j], axis=0, keepdims=True) for j in span]
        w_own = [e_own[j] * inv[j] for j in span]
        w_pri = [e_pri[j] * inv[j] for j in span]
        centred = [jnp.sum(w_own[j] * p_own[j] + w_pri[j] * p_pri[j], axis=0, keepdims=True) for j in span]
        sl_own = [((w_own[j] * (p_own[j] - centred[j])) * SCALE).astype(BF16) for j in span]
        sl_pri = [((w_pri[j] * (p_pri[j] - centred[j])) * SCALE).astype(BF16) for j in span]
        w_own = [w.astype(BF16) for w in w_own]
        w_pri = [w.astype(BF16) for w in w_pri]
        att, gq, dk, dv = [], [], [], []
        for j in span:
            pair = jnp.concatenate([kv[j - 1] if j else kv_last, kv[j]], axis=0)
            att.append(dot(jnp.concatenate([w_pri[j], w_own[j]], axis=0), pair[:, 128:256], 0, 0).astype(BF16))
            gq.append(dot(jnp.concatenate([sl_pri[j], sl_own[j]], axis=0), pair[:, 0:128], 0, 0).astype(BF16))
            dk.append(dot(jnp.concatenate([sl_own[j - 1] if j else sl_last, sl_pri[j]], axis=1),
                          jnp.concatenate([qs[j], qs[j + 1]], axis=0), 1, 0))
            dv.append(dot(jnp.concatenate([w_own[j - 1] if j else w_last, w_pri[j]], axis=1),
                          jnp.concatenate([os[j], os[j + 1]], axis=0), 1, 0))
        for j in span:
            at = slice(b[j] * 16, b[j] * 16 + 16)
            for h in range(8):
                to = slice((gi * 8 + h) * 128, (gi * 8 + h + 1) * 128)
                OP[at, to] = att[j][h * 16:(h + 1) * 16]
                DQP[at, to] = gq[j][h * 16:(h + 1) * 16]
        first = 0 if i else 1
        unseat(gi, dk[first:], dv[first:], [bj - 1 for bj in b[first:]])
        for j in span[first:]:
            total = total + jnp.sum(dv[j].reshape(16, 8, 128), axis=0)
        if i == GROUPS - 1:
            dk = dot(sl_own[-1], qs[un], 1, 0)
            dv = dot(w_own[-1], os[un], 1, 0)
            unseat(gi, [dk], [dv], [31])
            total = total + jnp.sum(dv.reshape(16, 8, 128), axis=0)
            BV[16 + gi:17 + gi, :] = jnp.sum(total, axis=0, keepdims=True)
        return s[-1][:, 128:256], p[-1][:, 128:256], w_own[-1], sl_own[-1], kv[-1], total

    def seen_at(b):
        return b % 2 * 16 + b // 16 * 8 + b // 2 % 8

    def opening():
        zf = jnp.zeros((128, 128), F32)
        zb = jnp.zeros((128, 128), BF16)
        return zf, zf, zb, zb, jnp.zeros((128, 256), BF16), jnp.zeros((8, 128), F32)

    def narrow(gi, places):
        out = []
        for far, zz in places:
            at = pl.ds(pl.multiple_of((side(far) * 8 + zz) * 16, 16), 16)
            wide = PAD[gi, 1:33, at, :].reshape(512, 256)
            out.append(dot(placing(side(far) * 8 + zz), wide, 0, 0).astype(BF16))
        for (far, zz), value in zip(places, out):
            D[gi, side(far), zz] = value

    back = {}

    def give(gi, far, s):
        item = 2 * far + gi
        if s == 0:
            jumps[gi].wait_recv()
            YX[gi] = (YX[gi].astype(F32) + D[gi, side(0), ring(z + 4)].astype(F32)).astype(BF16)
        for part in range(2):
            for way in range(2):
                at = half[part]
                term = D.at[gi, side(far), ring(z + 4 - s if way == 0 else z - 4 + s), at, :]
                if s == 0:
                    if part != way:
                        continue
                    src = YX.at[gi, at, :]
                elif s == 1 and (far or part != way):
                    src = term
                else:
                    back[(item, way, s - 1, part)].wait_recv()
                    src = R.at[item, way, s - 1, at, :]
                    src[...] = (src[...].astype(F32) + term[...].astype(F32)).astype(BF16)
                back[(item, way, s, part)] = remote(src, R.at[item, way, s, at, :], r_send.at[item, way, s, part],
                                                    r_recv.at[item, way, s, part], right if way == 0 else left)

    def total(gi, far, at):
        item = 2 * far + gi
        return (D[gi, side(far), z, at, :].astype(F32) + R[item, 0, 3, at, :].astype(F32)
                + R[item, 1, 3, at, :].astype(F32))

    def finish(gi, far):
        item = 2 * far + gi
        for way in range(2):
            for part in range(2):
                back[(item, way, 3, part)].wait_recv()
        if far:
            YS[gi] = total(gi, 1, slice(0, 256)).astype(BF16)
            ys[gi] = remote(YS.at[gi], YR.at[gi], v_send.at[gi], v_recv.at[gi], across)
            return
        ys[gi].wait_recv()
        KS[gi] = (total(gi, 0, theirs) + YR[gi, theirs, :].astype(F32)).astype(BF16)
        ks.append(remote(KS.at[gi], KR.at[gi], k_send.at[gi], k_recv.at[gi], partner))
        done = (total(gi, 0, mine) + YR[gi, mine, :].astype(F32)).astype(BF16)
        gk[:, cols((2 * c + gi) * 128, 128)] = done[:, 0:128]
        gv[:, cols((2 * c + gi) * 128, 128)] = done[:, 128:256]

    def start_reduce(gi):
        narrow(gi, [(1, ring(z + 4)), (1, ring(z + 3)), (1, ring(z + 5))])
        jumps[gi] = remote(D.at[gi, side(1), ring(z + 4)], YX.at[gi], x_send.at[gi], x_recv.at[gi], across)
        give(gi, 1, 1)
        narrow(gi, [(far, ring(z + i)) for i in (2, 6) for far in (1, 0)])
        narrow(gi, [(1, ring(z + 1)), (1, ring(z + 7)), (0, ring(z + 4)), (0, ring(z + 3)), (0, ring(z + 5))])
        narrow(gi, [(0, ring(z + 1)), (0, ring(z + 7)), (1, z), (0, z)])

    ks = []

    lead(0)
    lead(1)
    bring(0, 0, 0, later=True)
    bring(1, 0, 0, later=True)
    flags = [remote(LK.at[flag], LK.at[flag], l_send.at[i], l_recv.at[i], along_z[i]) for i in range(7)]
    tables()
    BV[...] = jnp.zeros_like(BV)
    zeros = jnp.zeros((16, 2048), BF16)
    for ref in (QP, GP):
        ref[0:16, :] = zeros
        ref[528:544, :] = zeros
    for gi in range(2):
        widen(gi, 0, [z])
    for i in (4, 5):
        local[i].wait()
        core[i].wait_recv()
    here = placing(chip)

    def spread(ref, src, j):
        at = slice(j * 256, (j + 1) * 256)
        ref[16:528, at] = dot(here, src[:, at], 1, 0).astype(BF16)

    for j in range(4):
        spread(QP, QX, j)
    bring(0, 0, 1)
    for copy in flags:
        copy.wait_recv()
    part = pl.ds(c * 16 + yh * 8, 8)
    flag_y = remote(LK.at[part], LK.at[part], l_send.at[7], l_recv.at[7], across)
    for j in range(4):
        spread(GP, GX, j)
    bring(1, 0, 1)
    for j in range(4, 8):
        spread(QP, QX, j)
    bring(0, 0, 2)
    bring(0, 1, 0)
    flag_y.wait_recv()
    part = pl.ds(c * 16, 16)
    flag_core = remote(LK.at[part], LK.at[part], l_send.at[8], l_recv.at[8], partner)
    for j in range(4, 8):
        spread(GP, GX, j)
    bring(0, 0, 3)
    bring(0, 1, 1)
    bring(0, 0, 4)
    bring(1, 0, 2)
    bring(0, 1, 2)
    flag_core.wait_recv()
    bring(1, 0, 3)
    bring(0, 1, 3)
    bring(1, 1, 0)
    bring(0, 1, 4)
    bring(1, 0, 4)
    carry = blocks(0, 0, opening())
    bring(1, 1, 1)
    carry = blocks(0, 1, carry)
    carry = blocks(0, 2, carry)
    bring(1, 1, 2)
    carry = blocks(0, 3, carry)
    start_reduce(0)
    bring(1, 1, 3)
    bring(1, 1, 4)
    carry = blocks(1, 0, opening())
    give(0, 1, 2)
    carry = blocks(1, 1, carry)
    carry = blocks(1, 2, carry)
    give(0, 1, 3)
    give(0, 0, 0)
    carry = blocks(1, 3, carry)
    start_reduce(1)
    give(0, 0, 1)
    here = placing(chip)
    for j in range(8):
        at = slice(j * 256, (j + 1) * 256)
        ATT[:, at] = dot(here, OP[:, at], 0, 0).astype(BF16)
        wide = dot(here, DQP[:, at], 0, 0)
        GQ[:, at] = wide.astype(BF16)
        sums = jnp.sum(wide, axis=0, keepdims=True)
        BV[2 * j:2 * j + 1, :] = sums[:, 0:128]
        BV[2 * j + 1:2 * j + 2, :] = sums[:, 128:256]
    outs = []
    for i, (src, dst) in enumerate(((ATT, att), (GQ, gq))):
        outs.append(copied(src.at[mine, :], dst.at[:, cols(c * 2048, 2048)], out_sem.at[i]))
        core.append(remote(src.at[theirs, :], dst.at[:, cols(c * 2048, 2048)], o_send.at[i], o_recv.at[i], partner))

    def share(buffer, place, line, base, value):
        buffer[place] = value
        return [remote(buffer.at[place], buffer.at[place], b_send.at[base + i], b_recv.at[base + i], device)
                for i, device in enumerate(line)]

    def summed(buffer, copies, count):
        for copy in copies:
            copy.wait_recv()
        value = buffer[0]
        for i in range(1, count):
            value = value + buffer[i]
        return value

    copies = share(BZ, z, along_z, 0, BV[...])
    give(1, 1, 2)
    finish(0, 1)
    give(0, 0, 2)
    copies = share(BY, y, along_y, 7, summed(BZ, copies, 8))
    give(1, 0, 0)
    give(1, 1, 3)
    give(1, 0, 1)
    give(0, 0, 3)
    finish(1, 1)
    give(1, 0, 2)
    copies = share(BX, x, along_x, 14, summed(BY, copies, 8))
    finish(0, 0)
    give(1, 0, 3)
    finish(1, 0)
    BM[...] = summed(BX, copies, 4) * (65536.0**-0.5)
    BT[c] = BM[...]
    last = remote(BM, BT.at[c], b_send.at[17], b_recv.at[17], partner)
    for gi in range(2):
        ks[gi].wait_recv()
        gk[:, cols((2 * other + gi) * 128, 128)] = KR[gi, :, 0:128]
        gv[:, cols((2 * other + gi) * 128, 128)] = KR[gi, :, 128:256]
    last.wait_recv()
    for i in range(2):
        bias[i * 16:i * 16 + 16, :] = BT[i, 0:16, :]
        bias[32 + 2 * i:34 + 2 * i, :] = BT[i, 16:18, :]
    for copy in core[6:]:
        copy.wait_recv()
    for copy in outs:
        copy.wait()
    for copy in sent:
        copy.wait_send()


def stepped(q, k, v, g, plan, first):
    dma = pltpu.SemaphoreType.DMA
    return pl.pallas_call(
        step_kernel,
        out_shape=(
            jax.ShapeDtypeStruct((128, 4096), BF16),
            jax.ShapeDtypeStruct((128, 4096), BF16),
            jax.ShapeDtypeStruct((128, 512), BF16),
            jax.ShapeDtypeStruct((128, 512), BF16),
            jax.ShapeDtypeStruct((36, 128), F32),
        ),
        in_specs=[HBM] * 4 + [VMEM] * 2,
        out_specs=(ANY, ANY, VMEM, VMEM, VMEM),
        scratch_shapes=[
            pltpu.VMEM((2, 2, 8, 256, 256), BF16),
            pltpu.VMEM((256, 2048), BF16),
            pltpu.VMEM((256, 2048), BF16),
            pltpu.VMEM((32, 1, 128), jnp.int32),
            pltpu.VMEM((32, 128), jnp.int32),
            pltpu.VMEM((32, 256), jnp.int32),
            pltpu.VMEM((32, 128), jnp.int32),
            pltpu.VMEM((2, 24, 128), F32),
            pltpu.VMEM((544, 2048), BF16),
            pltpu.VMEM((544, 2048), BF16),
            pltpu.VMEM((512, 2048), BF16),
            pltpu.VMEM((512, 2048), BF16),
            pltpu.VMEM((2, 33, 256, 256), BF16),
            pltpu.VMEM((2, 2, 8, 256, 256), BF16),
            pltpu.VMEM((256, 2048), BF16),
            pltpu.VMEM((256, 2048), BF16),
            pltpu.VMEM((24, 128), F32),
            pltpu.VMEM((4, 2, 4, 256, 256), BF16),
            pltpu.VMEM((2, 256, 256), BF16),
            pltpu.VMEM((2, 256, 256), BF16),
            pltpu.VMEM((2, 128, 256), BF16),
            pltpu.VMEM((2, 128, 256), BF16),
            pltpu.VMEM((8, 24, 128), F32),
            pltpu.VMEM((8, 24, 128), F32),
            pltpu.VMEM((4, 24, 128), F32),
            pltpu.VMEM((24, 128), F32),
            pltpu.VMEM((2, 256, 256), BF16),
            dma((6,)), dma((6,)), dma((6,)), dma((2,)), dma((2,)), dma((4, 2, 4, 2)), dma((4, 2, 4, 2)), dma((9,)), dma((9,)),
            dma((2,)), dma((2,)), dma((2,)), dma((2,)), dma((2,)), dma((2,)), dma((2,)), dma((4, 2, 4, 2)), dma((4, 2, 4, 2)),
            dma((18,)), dma((18,)), dma((2,)), dma((2,)), dma((2,)), dma((2,)),
        ],
        compiler_params=pltpu.CompilerParams(collective_id=0, has_side_effects=True, vmem_limit_bytes=LIMIT * 2**20),
        name="step",
    )(q, k, v, g, plan, first)


def place_kernel(*refs):
    kept, (arrive, leave) = refs[10:15], refs[15:]
    for way, sem in ((0, arrive), (1, leave)):
        copies = []
        for i in range(5):
            pair = (refs[i], kept[i]) if way == 0 else (kept[i], refs[i + 5])
            copies.append(pltpu.make_async_copy(pair[0], pair[1], sem.at[i]))
        if way == 0:
            for copy in copies:
                copy.start()
            first = copies
        else:
            for i in range(5):
                first[i].wait()
                copies[i].start()
            for copy in copies:
                copy.wait()


def placed(*values):
    return pl.pallas_call(
        place_kernel,
        out_shape=tuple(jax.ShapeDtypeStruct(value.shape, value.dtype) for value in values),
        in_specs=[HBM] * 5,
        out_specs=(HBM,) * 5,
        scratch_shapes=[pltpu.VMEM(value.shape, value.dtype) for value in values] + [pltpu.SemaphoreType.DMA((5,))] * 2,
        compiler_params=pltpu.CompilerParams(vmem_limit_bytes=LIMIT * 2**20),
        name="place",
    )(*values)


def local(query_rows, key_rows, value_rows, out_grad, destination, group_first):
    outs = stepped(query_rows, key_rows, value_rows, out_grad, destination.reshape(32, 128), group_first)
    att, gq, gk, gv, bias = placed(*outs)
    return att, gq, gk, gv, bias.reshape(4608)


def solution(mesh):
    rows = P(("dp", "ctx"), None)
    return jax.shard_map(
        local, mesh=mesh, in_specs=(rows, rows, rows, rows, P("dp", None), P("dp", "ctx")),
        out_specs=(rows, rows, rows, rows, P()), check_vma=False)
```
